128 devices in a mesh: rows: 8 (over x, core), cols: 16 (over y, z).
Axes of the slice: x: 4, y: 4, z: 4, core: 2. Of those that a mesh axis runs over, the one named last changes fastest.
Arguments:
- source_points: bfloat16 [262144, 128], P(('rows', 'cols')), may hold values from -3 to 3
- target_points: bfloat16 [262144, 128], P('cols'), may hold values from -3 to 3
- source_cluster: int32 [262144], P(('rows', 'cols')), may hold values from 0 to 8191, as said below
- target_cluster: int32 [262144], P('cols'), may hold values from 0 to 8191, as said below
- active_blocks: int32 [1024, 4], replicated, may hold values from 0 to 1023, as said below
- active_count: int32 [1024], replicated, may hold values from 1 to 4, as said below
- row_weight: float32 [262144], P(('rows', 'cols')), may hold values from -4 to 4
- col_weight: float32 [262144], P('cols'), may hold values from -4 to 4
Outputs:
- row_potential: float32 [262144], P(('rows', 'cols'))
- col_potential: float32 [262144], P('cols')
- row_adjoint: float32 [262144], P(('rows', 'cols'))
- col_adjoint: float32 [262144], P('cols')
The draws below stay inside these ranges and needn't reach their ends.
Inputs may be any that keep to these rules, and one draw needn't show every extreme that they name: `source_cluster`: never falling; the 2048 points of device d (its index along rows+cols) form clusters 64 * d to 64 * (d + 1) - 1, each of one point or more. `target_cluster`: never falling; the 16384 points of index c of cols form clusters 512 * c to 512 * (c + 1) - 1, each of one point or more. `active_blocks`: each row of 4 distinct column blocks lies within the 64 column blocks of one index of cols; the 8 row blocks of one device name pairwise different indices of cols; every column block is the first entry of exactly one row. Only the first active_count[q] entries of row q of active_blocks are active.
All inputs are finite; a program needn't handle non-finite values.
Results may differ from the reference program's by a relative error of at most 0.0003.
Values may be sent and summed in bfloat16 or wider, within the bound.
No kernel may reach another device: no remote copies, remote signals or barrier semaphores. Data moves between devices by JAX's collectives and lax.ppermute only.
A program may use at most 128 MiB of HBM per device.

```python
import jax
import jax.numpy as jnp
from jax import lax

D = 128
BLOCK = 256
ACT = 4
ITER_C = 4
PASSES = 2
ROWS_DEV = 2048
COLS_DEV = 16384
NPTS = 262144
RBD = 8
CBD = 64
NBLK = 1024
CL_DEV = 64
CLC_DEV = 512
NCL = 8192
N_ROWS = 8
N_COLS = 16
DEVICES = 128


def cluster_ids(seed_key, shards, length, clusters):

    def one_shard(shard_key, shard_index):
        boundaries = jnp.sort(jax.random.permutation(shard_key, length - 1)[:clusters - 1] + 1)
        labels = jnp.searchsorted(boundaries, jnp.arange(length), side='right')
        return labels.astype(jnp.int32) + shard_index * clusters
    shard_keys = jax.random.split(seed_key, shards)
    return jax.vmap(one_shard)(shard_keys, jnp.arange(shards, dtype=jnp.int32)).reshape(-1)


def cloud(seed_key, labels, clusters):
    centers = 0.3 * jax.random.normal(jax.random.fold_in(seed_key, 1), (clusters, D), jnp.float32)
    spread = 0.1 * jax.random.normal(jax.random.fold_in(seed_key, 2), (labels.shape[0], D), jnp.float32)
    return jnp.take(centers, labels, axis=0) + spread


def far_shift(seed_key, labels):
    offset = jax.random.randint(jax.random.fold_in(seed_key, 1), (), 0, 8)
    picked = (labels + offset) % 8 == 0
    strengths = jnp.array([150.0, 200.0, 250.0], jnp.float32)
    level = jax.random.randint(jax.random.fold_in(seed_key, 2), (NCL,), 0, 3)
    amount = jnp.sqrt(jnp.take(strengths, jnp.take(level, labels)) / D)
    return jnp.where(picked, amount, 0.0)[:, None]


def draw_source_cluster(key, part):
    return cluster_ids(jax.random.fold_in(key, 11), DEVICES, ROWS_DEV, CL_DEV)


def draw_target_cluster(key, part):
    return cluster_ids(jax.random.fold_in(key, 12), N_COLS, COLS_DEV, CLC_DEV)


def draw_source_points(key, part):
    labels = cluster_ids(jax.random.fold_in(key, 11), DEVICES, ROWS_DEV, CL_DEV)
    points = cloud(jax.random.fold_in(key, 21), labels, NCL)
    points = points + far_shift(jax.random.fold_in(key, 25), labels)
    return jnp.clip(points, -3.0, 3.0).astype(jnp.bfloat16)


def draw_target_points(key, part):
    labels = cluster_ids(jax.random.fold_in(key, 12), N_COLS, COLS_DEV, CLC_DEV)
    points = cloud(jax.random.fold_in(key, 22), labels, NCL)
    return jnp.clip(points, -3.0, 3.0).astype(jnp.bfloat16)


def active_plan(seed_key):
    base_key = jax.random.fold_in(seed_key, 29)
    row_order = jax.vmap(lambda sub_key: jax.random.permutation(sub_key, N_COLS)[:RBD])(jax.random.split(jax.random.fold_in(base_key, 1), N_ROWS))
    row_grid = jnp.arange(N_ROWS)[:, None, None]
    col_grid = jnp.arange(N_COLS)[None, :, None]
    slot_grid = jnp.arange(RBD)[None, None, :]
    owners = (col_grid + row_order[:, None, :]) % N_COLS
    slots = jnp.broadcast_to(row_grid * RBD + slot_grid, owners.shape)
    heads_table = jax.vmap(lambda sub_key: jax.random.permutation(sub_key, CBD))(jax.random.split(jax.random.fold_in(base_key, 2), N_COLS))
    heads = heads_table[owners, slots]
    local_heads = (heads[..., None] + jnp.arange(ACT)) % CBD
    blocks = (owners[..., None] * CBD + local_heads).reshape(-1, ACT).astype(jnp.int32)
    levels = jax.random.randint(jax.random.fold_in(base_key, 3), (DEVICES, 1), 1, ACT + 1)
    raw_draw = jax.random.randint(jax.random.fold_in(base_key, 4), (DEVICES, RBD), 0, ACT)
    counts = ACT - raw_draw % levels
    busiest = jax.random.randint(jax.random.fold_in(base_key, 5), (), 0, DEVICES)
    counts = jnp.where(jnp.arange(DEVICES)[:, None] == busiest, ACT, counts)
    lightest = jax.random.randint(jax.random.fold_in(base_key, 6), (), 0, DEVICES)
    first_slot = (jnp.arange(DEVICES)[:, None] == lightest) & (jnp.arange(RBD)[None, :] == 0)
    counts = jnp.where(first_slot, 1, counts)
    return (blocks, counts.reshape(-1).astype(jnp.int32))


def draw_active_blocks(key, part):
    return active_plan(key)[0]


def draw_active_count(key, part):
    return active_plan(key)[1]


def block_levels(own_key, dims, cuts, smallest, top_value):
    loudness, own = 1.0, jax.random.fold_in(own_key, 6)
    for dim, parts in cuts:
        steps = jnp.exp(jax.random.uniform(jax.random.fold_in(own, dim), (parts,), jnp.float32, smallest / len(cuts), top_value / len(cuts)))
        loudness = loudness * jnp.repeat(steps, dims[dim] // parts).reshape([-1 if axis == dim else 1 for axis in range(len(dims))])
    return loudness


def noise(rng, shape, deviation, reach, cuts=(), held_as=jnp.bfloat16):
    drawn = deviation * jax.random.normal(rng, shape, jnp.float32)
    if cuts:
        drawn = drawn * block_levels(rng, shape, cuts, -0.22, 0.18)
    return jnp.clip(drawn, -reach, reach).astype(held_as)


def setup_inputs(seed: int = 0) -> dict:
    splits = jax.random.split(jax.random.key(seed), 9)
    return {
        "source_points": draw_source_points(jax.random.fold_in(splits[8], 71), 0),
        "target_points": draw_target_points(jax.random.fold_in(splits[8], 71), 0),
        "source_cluster": draw_source_cluster(jax.random.fold_in(splits[8], 71), 0),
        "target_cluster": draw_target_cluster(jax.random.fold_in(splits[8], 71), 0),
        "active_blocks": draw_active_blocks(jax.random.fold_in(splits[8], 71), 0),
        "active_count": draw_active_count(jax.random.fold_in(splits[8], 71), 0),
        "row_weight": noise(splits[6], (NPTS,), 1.0, 4.0, ((0, 128),), jnp.float32),
        "col_weight": noise(splits[7], (NPTS,), 1.0, 4.0, ((0, 16),), jnp.float32),
    }


entropy_weight = 0.5
lowest = -1.0e30


def log_sum(scores, dimension):
    highest = jnp.max(scores, axis=dimension)
    return highest + jnp.log(jnp.sum(jnp.exp(scores - jnp.expand_dims(highest, dimension)), axis=dimension))


def lse_merge(former, latter):
    highest = jnp.maximum(former[0], latter[0])
    return (highest, former[1] * jnp.exp(former[0] - highest) + latter[1] * jnp.exp(latter[0] - highest))


def cluster_means(points, cluster, clusters):
    counts = jax.ops.segment_sum(jnp.ones((points.shape[0],), jnp.float32), cluster, num_segments=clusters)
    totals = jax.ops.segment_sum(points.astype(jnp.float32), cluster, num_segments=clusters)
    return totals / counts[:, None], counts


def half_norms(points):
    values = points.astype(jnp.float32)
    return 0.5 * jnp.sum(values * values, axis=-1)


def coarse_cost(sources, targets):
    products = jnp.dot(sources, targets.T, precision=lax.Precision.HIGHEST, preferred_element_type=jnp.float32)
    return half_norms(sources)[:, None] + half_norms(targets)[None, :] - products


def block_cost(row_points, row_half, col_points, col_half):
    products = jnp.einsum("id,ajd->iaj", row_points.astype(jnp.float32), col_points.astype(jnp.float32), precision=lax.Precision.HIGHEST)
    return row_half[:, None, None] + col_half[None, :, :] - products


def reference(source_points, target_points, source_cluster, target_cluster, active_blocks, active_count, row_weight, col_weight):
    src_mean, src_count = cluster_means(source_points, source_cluster, NCL)
    tgt_mean, tgt_count = cluster_means(target_points, target_cluster, NCL)
    coarse = coarse_cost(src_mean, tgt_mean)
    tgt_coarse = jnp.zeros((NCL,), jnp.float32)
    for sweep_index in range(ITER_C):
        src_coarse = entropy_weight * jnp.log(src_count) - entropy_weight * log_sum((tgt_coarse[None, :] - coarse) / entropy_weight, 1)
        tgt_coarse = entropy_weight * jnp.log(tgt_count) - entropy_weight * log_sum((src_coarse[:, None] - coarse) / entropy_weight, 0)
    col_values = jnp.take(tgt_coarse, target_cluster) - entropy_weight * jnp.log(jnp.take(tgt_count, target_cluster))

    row_blocks = source_points.reshape(NBLK, BLOCK, D)
    col_blocks = target_points.reshape(NBLK, BLOCK, D)
    row_half = half_norms(source_points).reshape(NBLK, BLOCK)
    col_half = half_norms(target_points).reshape(NBLK, BLOCK)
    active = jnp.arange(ACT)[None, :] < active_count[:, None]
    block_items = (row_blocks, row_half, active_blocks, active)
    row_weights = row_weight.reshape(NBLK, BLOCK)
    col_weights = col_weight.reshape(NBLK, BLOCK)

    def tile_costs(packed):
        return block_cost(packed[0], packed[1], jnp.take(col_blocks, packed[2], axis=0), jnp.take(col_half, packed[2], axis=0))

    col_grid = col_values.reshape(NBLK, BLOCK)
    row_grid = jnp.zeros((NBLK, BLOCK), jnp.float32)
    for pass_index in range(PASSES):
        def row_step(packed):
            scores = (jnp.take(col_grid, packed[2], axis=0)[None, :, :] - tile_costs(packed)) / entropy_weight
            scores = jnp.where(packed[3][None, :, None], scores, lowest)
            return -entropy_weight * log_sum(scores.reshape(BLOCK, -1), 1)

        row_grid = lax.map(row_step, block_items)

        def col_step(running, packed):
            block_packed, row_values = packed
            scores = (row_values[:, None, None] - tile_costs(block_packed)) / entropy_weight
            highest = jnp.max(scores, axis=0)
            mass_sum = jnp.sum(jnp.exp(scores - highest[None]), axis=0)
            highest = jnp.where(block_packed[3][:, None], highest, lowest)
            mass_sum = jnp.where(block_packed[3][:, None], mass_sum, 0.0)
            merged = lse_merge((jnp.take(running[0], block_packed[2], axis=0), jnp.take(running[1], block_packed[2], axis=0)), (highest, mass_sum))
            return (running[0].at[block_packed[2]].set(merged[0]), running[1].at[block_packed[2]].set(merged[1])), None

        initial = (jnp.full((NBLK, BLOCK), lowest, jnp.float32), jnp.zeros((NBLK, BLOCK), jnp.float32))
        (highest, mass_sum), unused = lax.scan(col_step, initial, (block_items, row_grid))
        col_grid = -entropy_weight * (highest + jnp.log(mass_sum))

    def plan_tile(packed, row_values):
        exponent = (row_values[:, None, None] + jnp.take(col_grid, packed[2], axis=0)[None, :, :]) - tile_costs(packed)
        return jnp.where(packed[3][None, :, None], jnp.exp(exponent / entropy_weight), 0.0)

    def row_adjoint_step(packed):
        block_packed, row_values, weights = packed
        plan_entries = plan_tile(block_packed, row_values)
        spread = jnp.take(col_weights, block_packed[2], axis=0)
        return weights * jnp.sum(plan_entries, axis=(1, 2)) + jnp.sum(plan_entries * spread[None], axis=(1, 2))

    row_adjoint = lax.map(row_adjoint_step, (block_items, row_grid, row_weights)).reshape(-1)

    def col_adjoint_step(running, packed):
        block_packed, row_values, weights = packed
        plan_entries = plan_tile(block_packed, row_values)
        return running.at[block_packed[2]].add(jnp.sum(plan_entries * weights[:, None, None], axis=0)), None

    col_sums, unused = lax.scan(col_adjoint_step, jnp.zeros((NBLK, BLOCK), jnp.float32), (block_items, row_grid, row_weights))
    col_adjoint = col_sums.reshape(-1) + col_weight
    return row_grid.reshape(-1), col_grid.reshape(-1), row_adjoint, col_adjoint
```

```python
import jax
import jax.numpy as jnp
from jax import lax
from jax.experimental import pallas as pl
from jax.experimental.pallas import tpu as pltpu
from jax.sharding import Mesh
from jax.sharding import PartitionSpec as P

D = 128
BLOCK = 256
ACT = 4
ITER_C = 4
CL_DEV = 64
RBD = 8
CBD = 64
ROWS = ("x", "core")
COLS = ("y", "z")
ALL = ("x", "core", "y", "z")
N_ROWS = 8
N_COLS = 16
N_SRC = CL_DEV * N_COLS
N_TGT = 512
PTS_SRC = 2048
PTS_TGT = 16384
WINDOW = 136

entropy_weight = 0.5
SCALE = 2.8853900817779268
lowest = -1.0e30
HI = lax.Precision.HIGHEST
NT = (((1,), (1,)), ((), ()))

VM = pl.BlockSpec(memory_space=pltpu.VMEM)
SM = pl.BlockSpec(memory_space=pltpu.SMEM)
ANY = pl.BlockSpec(memory_space=pl.ANY)


def shape(*dims, dtype=jnp.float32):
    return jax.ShapeDtypeStruct(dims, dtype)


def eye(rows, shift=0):
    return lax.broadcasted_iota(jnp.int32, (rows, 128), 0) + shift == lax.broadcasted_iota(
        jnp.int32, (rows, 128), 1
    )


def to_row(column, mask):
    return jnp.sum(jnp.where(mask, column, 0.0), axis=0, keepdims=True)


def to_column(row, mask):
    return jnp.sum(jnp.where(mask, row, 0.0), axis=1, keepdims=True)


def lse_list(parts):
    highest = parts[0]
    for part in parts[1:]:
        highest = jnp.maximum(highest, part)
    terms = [jnp.exp2(part - highest) for part in parts]
    while len(terms) > 1:
        terms = [terms[k] + terms[k + 1] for k in range(0, len(terms), 2)]
    return highest + jnp.log2(terms[0])


def one_hot(labels, rows):
    hit = lax.broadcasted_iota(jnp.int32, (rows, labels.shape[1]), 0) == labels
    return jnp.where(hit, 1.0, 0.0).astype(jnp.bfloat16)


def totals_and_counts(hits, points):
    both = jnp.concatenate([points, jnp.ones(points.shape, jnp.bfloat16)], axis=1)
    return jnp.dot(hits, both, preferred_element_type=jnp.float32)


def source_means_kernel(points, labels, out):
    both = totals_and_counts(one_hot(labels[...], CL_DEV), points[...])
    counts = both[:, D:]
    means = both[:, :D] / counts
    low = to_row(counts, eye(CL_DEV))
    high = to_row(counts, eye(CL_DEV, 64))
    tail = lax.broadcasted_iota(jnp.int32, (8, 128), 0)
    tail = jnp.where(tail == 0, low, jnp.where(tail == 1, high, 0.0))
    for peer in range(N_COLS):
        out[peer, :CL_DEV, :] = means
        out[peer, CL_DEV:, :] = tail


def target_means_kernel(points, labels, means, logs, acc):
    step = pl.program_id(0)

    @pl.when(step == 0)
    def _():
        acc[...] = jnp.zeros_like(acc)

    for part in range(4):
        at = slice(part * 512, (part + 1) * 512)
        acc[...] += totals_and_counts(one_hot(labels[0, :, at], N_TGT), points[at, :])

    @pl.when(step == pl.num_programs(0) - 1)
    def _():
        mask = eye(128)
        for part in range(4):
            at = slice(part * 128, (part + 1) * 128)
            counts = acc[at, D:]
            means[at, :] = acc[at, :D] / counts
            logs[:, at] = jnp.log2(to_row(counts, mask))


def row_lse_chunk(scores):
    highest = jnp.max(scores, axis=1, keepdims=True)
    return highest + jnp.log2(jnp.sum(jnp.exp2(scores - highest), axis=1, keepdims=True))


def coarse_start_kernel(gathered, targets, gains, source_logs, out):
    mask = eye(128)
    y = targets[...]
    half_y = 0.5 * jnp.sum(y * y, axis=1, keepdims=True)
    half_y = jnp.concatenate(
        [to_row(half_y[k * 128 : (k + 1) * 128], mask) for k in range(4)], axis=1
    )
    for part in range(8):
        x = jnp.concatenate(
            [gathered[2 * part, :CL_DEV, :], gathered[2 * part + 1, :CL_DEV, :]], axis=0
        )
        counts = gathered[2 * part, 64:65, :] + gathered[2 * part + 1, 65:66, :]
        source_logs[part : part + 1, :] = jnp.log2(counts)
        half_x = 0.5 * jnp.sum(x * x, axis=1, keepdims=True)
        products = lax.dot_general(x, y, NT, precision=HI, preferred_element_type=jnp.float32)
        gain = SCALE * (products - (half_x + half_y))
        gains[part * 128 : (part + 1) * 128, :] = gain
        out[0, part : part + 1, :] = to_row(row_lse_chunk(gain), mask)
    first = out[0]
    for peer in range(1, N_COLS):
        out[peer] = first


def coarse_rows_kernel(gathered, target_logs, gains, out):
    mask = eye(128)
    potential = target_logs[...] - lse_list([gathered[k] for k in range(N_ROWS)])
    for part in range(8):
        pieces = []
        for piece in range(2):
            at = part * 128 + piece * 64
            pieces.append(row_lse_chunk(gains[at : at + 64, :] + potential))
        out[0, part : part + 1, :] = to_row(jnp.concatenate(pieces, axis=0), mask)
    first = out[0]
    for peer in range(1, N_COLS):
        out[peer] = first


def coarse_cols_kernel(gathered, source_logs, gains, out, scores):
    mask = eye(128)
    potential = source_logs[...] - lse_list([gathered[k] for k in range(N_COLS)])
    highest = jnp.full((8, N_TGT), lowest, jnp.float32)
    for part in range(8):
        at = slice(part * 128, (part + 1) * 128)
        value = gains[at, :] + to_column(potential[part : part + 1, :], mask)
        scores[at, :] = value
        highest = jnp.maximum(highest, jnp.max(value.reshape(16, 8, N_TGT), axis=0))
    highest = jnp.max(highest, axis=0, keepdims=True)
    total = jnp.zeros((8, N_TGT), jnp.float32)
    for part in range(8):
        at = slice(part * 128, (part + 1) * 128)
        value = jnp.exp2(scores[at, :] - highest)
        total = total + jnp.sum(value.reshape(16, 8, N_TGT), axis=0)
    result = highest + jnp.log2(jnp.sum(total, axis=0, keepdims=True))
    for peer in range(N_ROWS):
        out[peer] = result


def start_copies(counts, blocks, x_hbm, y_hbm, xs, ys, sems):
    def copies(slot):
        found = [pltpu.make_async_copy(x_hbm.at[slot], xs.at[slot], sems.at[slot, ACT])]
        for a in range(ACT):
            first = pl.multiple_of(blocks[slot * ACT + a] * BLOCK, BLOCK)
            found.append(
                pltpu.make_async_copy(
                    y_hbm.at[pl.ds(first, BLOCK), :], ys.at[slot * ACT + a], sems.at[slot, a]
                )
            )
        return found

    def begin(slot, carry):
        @pl.when(counts[slot] > 0)
        def _():
            for copy in copies(slot):
                copy.start()

        return carry

    lax.fori_loop(0, N_COLS, begin, 0)
    return copies


def slot_products(slot, xs, ys, work):
    x = xs[slot]
    filler = jnp.full((BLOCK, 2 * D), -0.5, jnp.bfloat16)
    left = jnp.concatenate([x, filler], axis=1)
    for a in range(ACT):
        y = ys[slot * ACT + a]
        wide = y.astype(jnp.float32)
        square = wide * wide
        high = square.astype(jnp.bfloat16)
        low = (square - high.astype(jnp.float32)).astype(jnp.bfloat16)
        right = jnp.concatenate([y, high, low], axis=1)
        work[:, a * BLOCK : (a + 1) * BLOCK] = lax.dot_general(
            left, right, NT, preferred_element_type=jnp.float32
        )


def slot_potential(slot, counts, blocks, values):
    rows = []
    for a in range(ACT):
        row = values[blocks[slot * ACT + a]]
        rows.append(jnp.where(a < counts[slot], row, lowest))
    return jnp.concatenate(rows, axis=1)


CHUNK = 16
CHUNKS = BLOCK // CHUNK


def fine_slot(slot, counts, blocks, xs, ys, work, values, best, weights, mixed, lam_out, f_out):
    slot_products(slot, xs, ys, work)
    potential = slot_potential(slot, counts, blocks, values)
    mask = eye(128)
    width = ACT * BLOCK
    highest = jnp.full((8, width), lowest, jnp.float32)
    lams = []
    for k in range(CHUNKS):
        at = slice(k * CHUNK, (k + 1) * CHUNK)
        scores = SCALE * work[at, :] + potential
        lam = row_lse_chunk(scores)
        scores = scores - lam
        work[at, :] = scores
        highest = jnp.maximum(highest, jnp.max(scores.reshape(CHUNK // 8, 8, width), axis=0))
        lams.append(lam)
    highest = jnp.max(highest, axis=0, keepdims=True)
    total = jnp.zeros((8, width), jnp.float32)
    if weights is not None:
        w_row = weights[slot]
        w_cols = [to_column(w_row[:, h * 128 : (h + 1) * 128], mask) for h in range(2)]
        w_col = jnp.concatenate(w_cols, axis=0)
        weighted = jnp.zeros((8, width), jnp.float32)
    for k in range(CHUNKS):
        at = slice(k * CHUNK, (k + 1) * CHUNK)
        value = jnp.exp2(work[at, :] - highest)
        total = total + jnp.sum(value.reshape(CHUNK // 8, 8, width), axis=0)
        if weights is not None:
            value = value * w_col[at]
            weighted = weighted + jnp.sum(value.reshape(CHUNK // 8, 8, width), axis=0)
    total = jnp.sum(total, axis=0, keepdims=True)
    result = highest + jnp.log2(total)
    if weights is not None:
        mean = jnp.sum(weighted, axis=0, keepdims=True) / total
    for a in range(ACT):
        block = blocks[slot * ACT + a]
        at = slice(a * BLOCK, (a + 1) * BLOCK)
        here = jnp.where(a < counts[slot], result[:, at] - values[block], lowest)
        old = best[block]
        top = jnp.maximum(old, here)
        old_part, new_part = jnp.exp2(old - top), jnp.exp2(here - top)
        both = old_part + new_part
        best[block] = top + jnp.log2(both)
        if weights is not None:
            mixed[block] = (mixed[block] * old_part + mean[:, at] * new_part) / both
    if lam_out is not None:
        for h in range(2):
            at = slice(h * 128, (h + 1) * 128)
            lam = jnp.concatenate(lams[h * 8 : (h + 1) * 8], axis=0)
            wide = xs[slot, at, :].astype(jnp.float32)
            half_x = 0.5 * jnp.sum(wide * wide, axis=1, keepdims=True)
            lam_out[slot, :, at] = to_row(lam, mask)
            f_out[slot, :, at] = to_row(half_x - lam * (1.0 / SCALE), mask)


def clear(best, mixed=None):
    best[...] = jnp.full(best.shape, lowest, jnp.float32)
    if mixed is not None:
        mixed[...] = jnp.zeros(mixed.shape, jnp.float32)


def each_slot(counts, copies, body):
    def step(slot, carry):
        @pl.when(counts[slot] > 0)
        def _():
            for copy in copies(slot):
                copy.wait()
            body(slot)

        return carry

    lax.fori_loop(0, N_COLS, step, 0)


def first_pass_kernel(
    counts, blocks, starts, gathered, labels, x_hbm, y_hbm, best, values, table, work, xs, ys, sems
):
    copies = start_copies(counts, blocks, x_hbm, y_hbm, xs, ys, sems)
    clear(best)
    mask = eye(128)
    cluster_values = -lse_list([gathered[k] for k in range(N_ROWS)])
    for part in range(4):
        at = slice(part * 128, (part + 1) * 128)
        table[at, :] = jnp.broadcast_to(to_column(cluster_values[:, at], mask), (128, 128))

    def spread(block, carry):
        for h in range(2):
            first = pl.multiple_of(starts[2 * block + h], 8)
            at = slice(h * 128, (h + 1) * 128)
            index = lax.broadcasted_iota(jnp.int32, (WINDOW, 128), 0) + first
            hit = index == labels[block, :, at]
            window = table[pl.ds(first, WINDOW), :]
            values[block, :, at] = jnp.sum(jnp.where(hit, window, 0.0), axis=0, keepdims=True)
        return carry

    lax.fori_loop(0, CBD, spread, 0)
    each_slot(
        counts,
        copies,
        lambda slot: fine_slot(
            slot, counts, blocks, xs, ys, work, values, best, None, None, None, None
        ),
    )


def second_pass_kernel(
    counts, blocks, l0, l1, l2, l3, weights, x_hbm, y_hbm, both, lam, f, values, work, xs, ys, sems
):
    copies = start_copies(counts, blocks, x_hbm, y_hbm, xs, ys, sems)
    best, mixed = both.at[:CBD], both.at[CBD:]
    clear(best, mixed)
    values[...] = -lse_list([l0[...], l1[...], l2[...], l3[...]])
    each_slot(
        counts,
        copies,
        lambda slot: fine_slot(
            slot, counts, blocks, xs, ys, work, values, best, weights, mixed, lam, f
        ),
    )


def adjoint_kernel(
    counts, blocks, b0, b1, b2, b3, lam, f, weights, col_weights, x_hbm, y_hbm,
    potential_out, adjoint_out, back, values, work, xs, ys, sems,
):
    copies = start_copies(counts, blocks, x_hbm, y_hbm, xs, ys, sems)
    parts = [b0, b1, b2, b3]
    total = lse_list([part[:CBD] for part in parts])
    mixed = [part[CBD:] * jnp.exp2(part[:CBD] - total) for part in parts]
    mixed = (mixed[0] + mixed[1]) + (mixed[2] + mixed[3])
    values[...] = -total
    potential_out[...] = total * (-1.0 / SCALE)
    adjoint_out[...] = mixed + col_weights[...]
    back[...] = jnp.zeros(back.shape, jnp.float32)
    mask = eye(128)

    def body(slot):
        slot_products(slot, xs, ys, work)
        potential = slot_potential(slot, counts, blocks, values)
        spread = jnp.concatenate(
            [col_weights[blocks[slot * ACT + a]] for a in range(ACT)], axis=1
        )
        for h in range(2):
            half = slice(h * 128, (h + 1) * 128)
            shift = to_column(lam[slot, :, half], mask)
            sums, crossed = [], []
            for k in range(128 // CHUNK):
                at = slice(h * 128 + k * CHUNK, h * 128 + (k + 1) * CHUNK)
                scores = SCALE * work[at, :] + potential
                entries = jnp.exp2(scores - shift[k * CHUNK : (k + 1) * CHUNK])
                sums.append(jnp.sum(entries, axis=1, keepdims=True))
                crossed.append(jnp.sum(entries * spread, axis=1, keepdims=True))
            mass = to_row(jnp.concatenate(sums, axis=0), mask)
            cross = to_row(jnp.concatenate(crossed, axis=0), mask)
            back[slot, :, half] = f[slot, :, half]
            back[slot, :, BLOCK + h * 128 : BLOCK + (h + 1) * 128] = (
                weights[slot, :, half] * mass + cross
            )

    each_slot(counts, copies, body)


def spread_kernel(owners, x_hbm, out, sems):
    copies = [
        pltpu.make_async_copy(
            x_hbm.at[q * BLOCK : (q + 1) * BLOCK, :], out.at[owners[q]], sems.at[q]
        )
        for q in range(RBD)
    ]
    for copy in copies:
        copy.start()
    for copy in copies:
        copy.wait()


FINE_SCRATCH = (
    pltpu.VMEM((CBD, 1, BLOCK), jnp.float32),
    pltpu.VMEM((BLOCK, ACT * BLOCK), jnp.float32),
    pltpu.VMEM((N_COLS, BLOCK, D), jnp.bfloat16),
    pltpu.VMEM((N_COLS * ACT, BLOCK, D), jnp.bfloat16),
    pltpu.SemaphoreType.DMA((N_COLS, ACT + 1)),
)


def cost(flops):
    return pl.CostEstimate(flops=int(flops), transcendentals=0, bytes_accessed=4 << 20)


def exchange(x, axis):
    return lax.all_to_all(x, axis, split_axis=0, concat_axis=0, tiled=True)


def partner(x, axis, step):
    n = lax.axis_size(axis)
    return lax.ppermute(x, axis, [(k, k ^ step) for k in range(n)])


def four_along_x(x):
    return [x] + [partner(x, "x", step) for step in (1, 2, 3)]


def on_device(
    source_points,
    target_points,
    source_cluster,
    target_cluster,
    active_blocks,
    active_count,
    row_weight,
    col_weight,
):
    row_index = lax.axis_index(ROWS)
    col_index = lax.axis_index(COLS)
    device = row_index * N_COLS + col_index

    group = lax.dynamic_slice_in_dim(active_blocks, row_index * N_COLS * RBD, N_COLS * RBD, 0)
    group_count = lax.dynamic_slice_in_dim(active_count, row_index * N_COLS * RBD, N_COLS * RBD)
    group_count = group_count.reshape(N_COLS, RBD)
    group = group.reshape(N_COLS, RBD, ACT)
    owners = group[:, :, 0] // CBD
    hit = owners == col_index
    blocks = jnp.sum(jnp.where(hit[:, :, None], group % CBD, 0), axis=1).reshape(-1)
    counts = jnp.sum(jnp.where(hit, group_count, 0), axis=1)
    my_owners = lax.dynamic_slice_in_dim(owners, col_index, 1, 0)[0]

    row_weights = row_weight.reshape(RBD, BLOCK)
    col_weights = col_weight.reshape(CBD, 1, BLOCK)
    mine = my_owners[None, :] == jnp.arange(N_COLS)[:, None]
    sent_weights = jnp.sum(jnp.where(mine[:, :, None], row_weights[None], 0.0), axis=1)
    sent_points = pl.pallas_call(
        spread_kernel,
        out_shape=shape(N_COLS, BLOCK, D, dtype=jnp.bfloat16),
        in_specs=[SM, ANY],
        out_specs=ANY,
        scratch_shapes=[pltpu.SemaphoreType.DMA((RBD,))],
        name="spread_points",
    )(my_owners, source_points)

    packed = pl.pallas_call(
        source_means_kernel,
        out_shape=shape(N_COLS, CL_DEV + 8, D),
        in_specs=[VM, VM],
        out_specs=VM,
        name="source_means",
    )(source_points, (source_cluster - CL_DEV * device).reshape(1, PTS_SRC))
    gathered = exchange(packed, COLS)
    points_here = exchange(sent_points, COLS)
    weights_here = exchange(sent_weights.reshape(N_COLS, 1, BLOCK), COLS)

    labels = target_cluster - N_TGT * col_index
    target_means, target_logs = pl.pallas_call(
        target_means_kernel,
        out_shape=(shape(N_TGT, D), shape(1, N_TGT)),
        grid=(8,),
        in_specs=[
            pl.BlockSpec((2048, D), lambda k: (k, 0)),
            pl.BlockSpec((1, 1, 2048), lambda k: (k, 0, 0)),
        ],
        out_specs=(
            pl.BlockSpec((N_TGT, D), lambda k: (0, 0)),
            pl.BlockSpec((1, N_TGT), lambda k: (0, 0)),
        ),
        scratch_shapes=[pltpu.VMEM((N_TGT, 2 * D), jnp.float32)],
        cost_estimate=cost(1e9),
        name="target_means",
    )(target_points, labels.reshape(8, 1, 2048))

    gains, source_logs, partial = pl.pallas_call(
        coarse_start_kernel,
        out_shape=(shape(N_SRC, N_TGT), shape(8, 128), shape(N_COLS, 8, 128)),
        in_specs=[VM, VM],
        out_specs=(VM, VM, VM),
        cost_estimate=cost(1e9),
        name="coarse_start",
    )(gathered, target_means)
    coarse_cols = pl.pallas_call(
        coarse_cols_kernel,
        out_shape=shape(N_ROWS, 1, N_TGT),
        in_specs=[VM, VM, VM],
        out_specs=VM,
        scratch_shapes=[pltpu.VMEM((N_SRC, N_TGT), jnp.float32)],
        cost_estimate=cost(1e8),
        name="coarse_cols",
    )
    coarse_rows = pl.pallas_call(
        coarse_rows_kernel,
        out_shape=shape(N_COLS, 8, 128),
        in_specs=[VM, VM, VM],
        out_specs=VM,
        cost_estimate=cost(1e8),
        name="coarse_rows",
    )
    for sweep in range(ITER_C):
        cols_partial = coarse_cols(exchange(partial, COLS), source_logs, gains)
        target_parts = exchange(cols_partial, ROWS)
        if sweep + 1 < ITER_C:
            partial = coarse_rows(target_parts, target_logs, gains)

    starts = jnp.minimum(labels.reshape(128, 128)[:, 0] // 8 * 8, N_TGT - WINDOW)
    column = shape(CBD, 1, BLOCK)
    best = pl.pallas_call(
        first_pass_kernel,
        out_shape=column,
        in_specs=[SM, SM, SM, VM, VM, ANY, ANY],
        out_specs=VM,
        scratch_shapes=[
            FINE_SCRATCH[0],
            pltpu.VMEM((N_TGT, 128), jnp.float32),
            *FINE_SCRATCH[1:],
        ],
        cost_estimate=cost(1e9),
        name="first_pass",
    )(counts, blocks, starts, target_parts, labels.reshape(CBD, 1, BLOCK), points_here, target_points)
    other = partner(best, "core", 1)
    best = lse_list([best, other])

    slot_row = shape(N_COLS, 1, BLOCK)
    both, lam, f = pl.pallas_call(
        second_pass_kernel,
        out_shape=(shape(2 * CBD, 1, BLOCK), slot_row, slot_row),
        in_specs=[SM, SM, VM, VM, VM, VM, VM, ANY, ANY],
        out_specs=(VM, VM, VM),
        scratch_shapes=FINE_SCRATCH,
        cost_estimate=cost(1e9),
        name="second_pass",
    )(counts, blocks, *four_along_x(best), weights_here, points_here, target_points)
    other = partner(both, "core", 1)
    old, new = both[:CBD], other[:CBD]
    total = lse_list([old, new])
    mixed = both[CBD:] * jnp.exp2(old - total) + other[CBD:] * jnp.exp2(new - total)
    both = jnp.concatenate([total, mixed], axis=0)

    col_potential, col_adjoint, back = pl.pallas_call(
        adjoint_kernel,
        out_shape=(column, column, shape(N_COLS, 1, 2 * BLOCK)),
        in_specs=[SM, SM, VM, VM, VM, VM, VM, VM, VM, VM, ANY, ANY],
        out_specs=(VM, VM, VM),
        scratch_shapes=FINE_SCRATCH,
        cost_estimate=cost(1e9),
        name="adjoint",
    )(
        counts, blocks, *four_along_x(both), lam, f, weights_here, col_weights,
        points_here, target_points,
    )
    back = exchange(back, COLS).reshape(N_COLS, 2 * BLOCK)
    chosen = my_owners[:, None] == jnp.arange(N_COLS)[None, :]
    back = jnp.sum(jnp.where(chosen[:, :, None], back[None], 0.0), axis=1)
    return (
        back[:, :BLOCK].reshape(-1),
        col_potential.reshape(-1),
        back[:, BLOCK:].reshape(-1),
        col_adjoint.reshape(-1),
    )


def solution(mesh):
    split = Mesh(mesh.devices.reshape(4, 2, 4, 4), ALL)
    placed = (
        P(ALL, None),
        P(COLS, None),
        P(ALL),
        P(COLS),
        P(),
        P(),
        P(ALL),
        P(COLS),
    )
    return jax.shard_map(
        on_device,
        mesh=split,
        in_specs=placed,
        out_specs=(P(ALL), P(COLS), P(ALL), P(COLS)),
        check_vma=False,
    )
```

```python
import jax
import jax.numpy as jnp
from jax import lax
from jax.experimental import pallas as pl
from jax.experimental.pallas import tpu as pltpu
from jax.sharding import Mesh
from jax.sharding import PartitionSpec as P


D = 128
BLOCK = 256
ACT = 4
ITER_C = 4
CL_DEV = 64
RBD = 8
CBD = 64
ROWS = ("x", "core")
COLS = ("y", "z")
ALL = ("x", "core", "y", "z")
N_ROWS = 8
N_COLS = 16
N_SRC = CL_DEV * N_COLS
N_TGT = 512
PTS_SRC = 2048
WINDOW = 136
PIECE = 32
PACKED = BLOCK + 16

SCALE = 2.8853900817779268
lowest = -1.0e30
HI = lax.Precision.HIGHEST
NT = (((1,), (1,)), ((), ()))

VM = pl.BlockSpec(memory_space=pltpu.VMEM)
SM = pl.BlockSpec(memory_space=pltpu.SMEM)
ANY = pl.BlockSpec(memory_space=pl.ANY)


def vmem_shape(*dims, dtype=jnp.float32):
    return pltpu.VMEM(dims, dtype)


def in_vmem(x):
    return pltpu.with_memory_space_constraint(x, pltpu.VMEM)


def in_hbm(x):
    return pltpu.with_memory_space_constraint(x, pltpu.HBM)


def eye(rows, shift=0):
    return lax.broadcasted_iota(jnp.int32, (rows, 128), 0) + shift == lax.broadcasted_iota(
        jnp.int32, (rows, 128), 1
    )


def to_row(column, mask):
    return jnp.sum(jnp.where(mask, column, 0.0), axis=0, keepdims=True)


def to_column(row, mask):
    return jnp.sum(jnp.where(mask, row, 0.0), axis=1, keepdims=True)


def lse_list(parts):
    highest = parts[0]
    for part in parts[1:]:
        highest = jnp.maximum(highest, part)
    terms = [jnp.exp2(part - highest) for part in parts]
    while len(terms) > 1:
        terms = [terms[k] + terms[k + 1] for k in range(0, len(terms), 2)]
    return highest + jnp.log2(terms[0])


def one_hot(labels, rows):
    hit = lax.broadcasted_iota(jnp.int32, (rows, labels.shape[1]), 0) == labels
    return jnp.where(hit, 1.0, 0.0).astype(jnp.bfloat16)


def totals_and_counts(hits, points):
    both = jnp.concatenate([points, jnp.ones(points.shape, jnp.bfloat16)], axis=1)
    return jnp.dot(hits, both, preferred_element_type=jnp.float32)


def source_means_kernel(base, points, labels, out):
    both = totals_and_counts(one_hot(labels[...] - base[0], CL_DEV), points[...])
    counts = both[:, D:]
    means = both[:, :D] / counts
    low = to_row(counts, eye(CL_DEV))
    high = to_row(counts, eye(CL_DEV, 64))
    tail = lax.broadcasted_iota(jnp.int32, (8, 128), 0)
    tail = jnp.where(tail == 0, low, jnp.where(tail == 1, high, 0.0))
    for peer in range(N_COLS):
        out[peer, :CL_DEV, :] = means
        out[peer, CL_DEV:, :] = tail


def target_means_kernel(base, firsts, points, labels, means, logs, acc):
    step = pl.program_id(0)

    @pl.when(step == 0)
    def _():
        acc[...] = jnp.zeros_like(acc)

    def piece(chunk, start, points_here):
        at = slice(chunk * 256, (chunk + 1) * 256)
        hits = one_hot(labels[0, :, at] - (start + base[0]), PIECE)
        window = pl.ds(pl.multiple_of(start, 8), PIECE)
        acc[window, :] += totals_and_counts(hits, points_here)

    starts, extra = [], []
    for chunk in range(8):
        index = 2 * (step * 8 + chunk)
        start = firsts[index] // 8 * 8
        beyond = jnp.where(index + 2 < 128, firsts[jnp.minimum(index + 2, 127)], N_TGT - 1)
        starts.append(start)
        extra.append((beyond - start) // PIECE)
        piece(chunk, start, points[chunk * 256 : (chunk + 1) * 256, :])
    for chunk in range(8):
        def more(k, carry, chunk=chunk):
            piece(chunk, starts[chunk] + k * PIECE, points[chunk * 256 : (chunk + 1) * 256, :])
            return carry

        lax.fori_loop(1, extra[chunk] + 1, more, 0)

    @pl.when(step == pl.num_programs(0) - 1)
    def _():
        mask = eye(128)
        for part in range(4):
            at = slice(part * 128, (part + 1) * 128)
            counts = acc[at, D:]
            means[at, :] = acc[at, :D] / counts
            logs[:, at] = jnp.log2(to_row(counts, mask))


def row_lse_chunk(scores):
    highest = jnp.max(scores, axis=1, keepdims=True)
    return highest + jnp.log2(jnp.sum(jnp.exp2(scores - highest), axis=1, keepdims=True))


def coarse_start_kernel(gathered, targets, gains, source_logs, out):
    mask = eye(128)
    y = targets[...]
    half_y = 0.5 * jnp.sum(y * y, axis=1, keepdims=True)
    half_y = jnp.concatenate(
        [to_row(half_y[k * 128 : (k + 1) * 128], mask) for k in range(4)], axis=1
    )
    for part in range(8):
        x = jnp.concatenate(
            [gathered[2 * part, :CL_DEV, :], gathered[2 * part + 1, :CL_DEV, :]], axis=0
        )
        counts = gathered[2 * part, 64:65, :] + gathered[2 * part + 1, 65:66, :]
        source_logs[part : part + 1, :] = jnp.log2(counts)
        half_x = 0.5 * jnp.sum(x * x, axis=1, keepdims=True)
        products = lax.dot_general(x, y, NT, precision=HI, preferred_element_type=jnp.float32)
        gain = SCALE * (products - (half_x + half_y))
        gains[part * 128 : (part + 1) * 128, :] = gain
        out[0, part : part + 1, :] = to_row(row_lse_chunk(gain), mask)
    first = out[0]
    for peer in range(1, N_COLS):
        out[peer] = first


def parts_of(refs):
    if len(refs) == 1:
        return [refs[0][k] for k in range(refs[0].shape[0])]
    return [ref[...] for ref in refs]


def coarse_rows_kernel(*refs):
    *gathered, target_logs, gains, out = refs
    mask = eye(128)
    potential = target_logs[...] - lse_list(parts_of(gathered))
    for part in range(8):
        pieces = []
        for piece in range(2):
            at = part * 128 + piece * 64
            pieces.append(row_lse_chunk(gains[at : at + 64, :] + potential))
        out[0, part : part + 1, :] = to_row(jnp.concatenate(pieces, axis=0), mask)
    first = out[0]
    for peer in range(1, N_COLS):
        out[peer] = first


def coarse_cols_kernel(*refs):
    *gathered, source_logs, gains, out, scores = refs
    mask = eye(128)
    potential = source_logs[...] - lse_list(parts_of(gathered))
    highest = jnp.full((8, N_TGT), lowest, jnp.float32)
    for part in range(8):
        at = slice(part * 128, (part + 1) * 128)
        value = gains[at, :] + to_column(potential[part : part + 1, :], mask)
        scores[at, :] = value
        highest = jnp.maximum(highest, jnp.max(value.reshape(16, 8, N_TGT), axis=0))
    highest = jnp.max(highest, axis=0, keepdims=True)
    total = jnp.zeros((8, N_TGT), jnp.float32)
    for part in range(8):
        at = slice(part * 128, (part + 1) * 128)
        value = jnp.exp2(scores[at, :] - highest)
        total = total + jnp.sum(value.reshape(16, 8, N_TGT), axis=0)
    result = highest + jnp.log2(jnp.sum(total, axis=0, keepdims=True))
    if len(out.shape) == 2:
        out[...] = result
    else:
        for peer in range(N_ROWS):
            out[peer] = result


def start_copies(counts, blocks, x_hbm, y_hbm, xs, ys, sems):
    def copies(slot):
        found = [pltpu.make_async_copy(x_hbm.at[slot], xs.at[slot], sems.at[slot, ACT])]
        for a in range(ACT):
            first = pl.multiple_of(blocks[slot * ACT + a] * BLOCK, BLOCK)
            found.append(
                pltpu.make_async_copy(
                    y_hbm.at[pl.ds(first, BLOCK), :], ys.at[slot * ACT + a], sems.at[slot, a]
                )
            )
        return found

    def begin(slot, carry):
        @pl.when(counts[slot] > 0)
        def _():
            for copy in copies(slot):
                copy.start()

        return carry

    lax.fori_loop(0, N_COLS, begin, 0)
    return copies


def half_norms_kernel(points, out):
    left = jnp.full((8, 2 * D), 1.0, jnp.bfloat16)
    for b in range(8):
        wide = points[b * BLOCK : (b + 1) * BLOCK, :].astype(jnp.float32)
        square = wide * wide
        high = square.astype(jnp.bfloat16)
        low = (square - high.astype(jnp.float32)).astype(jnp.bfloat16)
        right = jnp.concatenate([high, low], axis=1)
        total = lax.dot_general(left, right, NT, preferred_element_type=jnp.float32)
        out[b] = (0.5 * SCALE) * total[:1]


def products_kernel(counts, blocks, norms, x_hbm, y_hbm, gains, halves, weights, xs, ys, sems):
    copies = start_copies(counts, blocks, x_hbm, y_hbm, xs, ys, sems)
    mask = eye(128)

    def body(slot):
        x = xs[slot, :BLOCK, :]
        tail = xs[slot, BLOCK:, :].astype(jnp.float32)
        for h in range(2):
            at = slice(h * 128, (h + 1) * 128)
            wide = xs[slot, at, :].astype(jnp.float32)
            half_x = 0.5 * jnp.sum(wide * wide, axis=1, keepdims=True)
            halves[slot, :, at] = to_row(half_x, mask)
            weights[slot, :, at] = (tail[h : h + 1] + tail[h + 2 : h + 3]) + tail[h + 4 : h + 5]
        for a in range(ACT):
            products = lax.dot_general(
                x, ys[slot * ACT + a], NT, preferred_element_type=jnp.float32
            )
            gains[slot, :, a * BLOCK : (a + 1) * BLOCK] = (
                SCALE * products - norms[blocks[slot * ACT + a]]
            )

    each_slot(counts, body, copies)


def slot_potential(slot, counts, blocks, values):
    rows = []
    for a in range(ACT):
        row = values[blocks[slot * ACT + a]]
        rows.append(jnp.where(a < counts[slot], row, lowest))
    return jnp.concatenate(rows, axis=1)


CHUNK = 16
CHUNKS = BLOCK // CHUNK
WIDTH = ACT * BLOCK


def fine_slot(slot, counts, blocks, gains, work, values, best, weights=None, mixed=None, lam_out=None):
    potential = slot_potential(slot, counts, blocks, values)
    mask = eye(128)
    highest = jnp.full((8, WIDTH), lowest, jnp.float32)
    lams = []
    for k in range(CHUNKS):
        at = slice(k * CHUNK, (k + 1) * CHUNK)
        scores = gains[slot, at, :] + potential
        lam = row_lse_chunk(scores)
        scores = scores - lam
        work[at, :] = scores
        highest = jnp.maximum(highest, jnp.max(scores.reshape(CHUNK // 8, 8, WIDTH), axis=0))
        lams.append(lam)
    highest = jnp.max(highest, axis=0, keepdims=True)
    total = jnp.zeros((8, WIDTH), jnp.float32)
    if weights is not None:
        w_row = weights[slot]
        w_cols = [to_column(w_row[:, h * 128 : (h + 1) * 128], mask) for h in range(2)]
        w_col = jnp.concatenate(w_cols, axis=0)
        weighted = jnp.zeros((8, WIDTH), jnp.float32)
    for k in range(CHUNKS):
        at = slice(k * CHUNK, (k + 1) * CHUNK)
        value = jnp.exp2(work[at, :] - highest)
        total = total + jnp.sum(value.reshape(CHUNK // 8, 8, WIDTH), axis=0)
        if weights is not None:
            value = value * w_col[at]
            weighted = weighted + jnp.sum(value.reshape(CHUNK // 8, 8, WIDTH), axis=0)
    total = jnp.sum(total, axis=0, keepdims=True)
    result = highest + jnp.log2(total)
    if weights is not None:
        mean = jnp.sum(weighted, axis=0, keepdims=True) / total
    for a in range(ACT):
        block = blocks[slot * ACT + a]
        at = slice(a * BLOCK, (a + 1) * BLOCK)
        here = jnp.where(a < counts[slot], result[:, at] - values[block], lowest)
        old = best[block]
        top = jnp.maximum(old, here)
        old_part, new_part = jnp.exp2(old - top), jnp.exp2(here - top)
        both = old_part + new_part
        best[block] = top + jnp.log2(both)
        if weights is not None:
            mixed[block] = (mixed[block] * old_part + mean[:, at] * new_part) / both
    if lam_out is not None:
        for h in range(2):
            at = slice(h * 128, (h + 1) * 128)
            lam_out[slot, :, at] = to_row(jnp.concatenate(lams[h * 8 : (h + 1) * 8], axis=0), mask)


def clear(best, mixed=None):
    best[...] = jnp.full(best.shape, lowest, jnp.float32)
    if mixed is not None:
        mixed[...] = jnp.zeros(mixed.shape, jnp.float32)


def each_slot(counts, body, copies=None):
    def step(slot, carry):
        @pl.when(counts[slot] > 0)
        def _():
            if copies is not None:
                for copy in copies(slot):
                    copy.wait()
            body(slot)

        return carry

    lax.fori_loop(0, N_COLS, step, 0)


def first_pass_kernel(
    base, counts, blocks, starts, p0, p1, p2, p3, labels, gains, best, kept, values, table, work
):
    clear(best)
    mask = eye(128)
    cluster_values = -lse_list([p0[...], p1[...], p2[...], p3[...]])
    for part in range(4):
        at = slice(part * 128, (part + 1) * 128)
        table[at, :] = jnp.broadcast_to(to_column(cluster_values[:, at], mask), (128, 128))

    def spread(step, carry):
        for n in range(8):
            block, h = step * 4 + n // 2, n % 2
            first = starts[2 * block + h] // 8 * 8
            first = pl.multiple_of(jnp.minimum(first, N_TGT - WINDOW), 8)
            at = slice(h * 128, (h + 1) * 128)
            index = lax.broadcasted_iota(jnp.int32, (WINDOW, 128), 0)
            hit = index == labels[block, :, at] - (base[0] + first)
            window = table[pl.ds(first, WINDOW), :]
            values[block, :, at] = jnp.sum(jnp.where(hit, window, 0.0), axis=0, keepdims=True)
        return carry

    lax.fori_loop(0, CBD // 4, spread, 0)
    each_slot(
        counts, lambda slot: fine_slot(slot, counts, blocks, gains, work, values, best)
    )


def second_pass_kernel(
    counts, blocks, l0, l1, l2, l3, weights, gains, both, lam, kept, values, work
):
    best, mixed = both.at[:CBD], both.at[CBD:]
    clear(best, mixed)
    values[...] = -lse_list([l0[...], l1[...], l2[...], l3[...]])
    each_slot(
        counts,
        lambda slot: fine_slot(
            slot, counts, blocks, gains, work, values, best, weights, mixed, lam
        ),
    )


def adjoint_kernel(
    counts, blocks, b0, b1, b2, b3, lam, halves, weights, col_weights, gains,
    potential_out, adjoint_out, back, values,
):
    parts = [b0, b1, b2, b3]
    total = lse_list([part[:CBD] for part in parts])
    mixed = [part[CBD:] * jnp.exp2(part[:CBD] - total) for part in parts]
    mixed = (mixed[0] + mixed[1]) + (mixed[2] + mixed[3])
    values[...] = -total
    potential_out[...] = total * (-1.0 / SCALE)
    adjoint_out[...] = mixed + col_weights[...]
    back[...] = jnp.zeros(back.shape, jnp.float32)
    mask = eye(128)

    def body(slot):
        potential = slot_potential(slot, counts, blocks, values)
        spread = jnp.concatenate(
            [col_weights[blocks[slot * ACT + a]] for a in range(ACT)], axis=1
        )
        for h in range(2):
            half = slice(h * 128, (h + 1) * 128)
            shift = to_column(lam[slot, :, half], mask)
            sums, crossed = [], []
            for k in range(128 // CHUNK):
                at = slice(h * 128 + k * CHUNK, h * 128 + (k + 1) * CHUNK)
                scores = gains[slot, at, :] + potential
                entries = jnp.exp2(scores - shift[k * CHUNK : (k + 1) * CHUNK])
                sums.append(jnp.sum(entries, axis=1, keepdims=True))
                crossed.append(jnp.sum(entries * spread, axis=1, keepdims=True))
            mass = to_row(jnp.concatenate(sums, axis=0), mask)
            cross = to_row(jnp.concatenate(crossed, axis=0), mask)
            back[slot, :, half] = halves[slot, :, half] - lam[slot, :, half] * (1.0 / SCALE)
            back[slot, :, BLOCK + h * 128 : BLOCK + (h + 1) * 128] = (
                weights[slot, :, half] * mass + cross
            )

    each_slot(counts, body)


def spread_kernel(owners, points, weights, out):
    for q in range(RBD):
        owner = owners[q] // CBD
        out[owner, :BLOCK, :] = points[q * BLOCK : (q + 1) * BLOCK, :]
        rest = weights[q]
        pieces = []
        for _ in range(3):
            piece = rest.astype(jnp.bfloat16)
            rest = rest - piece.astype(jnp.float32)
            pieces.append(piece.astype(jnp.float32))
        pieces.append(jnp.zeros((10, D), jnp.float32))
        out[owner, BLOCK:, :] = jnp.concatenate(pieces, axis=0).astype(jnp.bfloat16)


def cost(flops):
    return pl.CostEstimate(flops=int(flops), transcendentals=0, bytes_accessed=4 << 20)


def call(kernel, out_shape, in_specs, scratch=(), flops=1e8, **kw):
    out_specs = jax.tree.map(lambda _: VM, out_shape, is_leaf=lambda x: hasattr(x, "shape"))
    return pl.pallas_call(
        kernel,
        out_shape=out_shape,
        in_specs=in_specs,
        out_specs=out_specs,
        scratch_shapes=list(scratch),
        compiler_params=pltpu.CompilerParams(vmem_limit_bytes=24 << 20),
        cost_estimate=cost(flops),
        **kw,
    )


def exchange(x, axis):
    return lax.all_to_all(x, axis, split_axis=0, concat_axis=0, tiled=True)


def partner(x, axis, step):
    n = lax.axis_size(axis)
    return lax.ppermute(x, axis, [(k, k ^ step) for k in range(n)])


def four_along(x, axis):
    found = [x]
    for step in (1, 2, 3):
        found.append(partner(x, axis, step))
    return found


def four_along_x(x):
    return [in_vmem(part) for part in four_along(x, "x")]


def on_device(
    source_points,
    target_points,
    source_cluster,
    target_cluster,
    active_blocks,
    active_count,
    row_weight,
    col_weight,
):
    row_index = lax.axis_index(ROWS)
    col_index = lax.axis_index(COLS)
    device = row_index * N_COLS + col_index

    source_base = (CL_DEV * device).reshape(1).astype(jnp.int32)
    target_base = (N_TGT * col_index).reshape(1).astype(jnp.int32)
    packed = call(
        source_means_kernel, vmem_shape(N_COLS, CL_DEV + 8, D), [SM, VM, VM]
    )(source_base, in_hbm(source_points), in_hbm(source_cluster.reshape(1, PTS_SRC)))
    gathered = exchange(packed, COLS)

    row_weights = row_weight.reshape(RBD, 2, 128)
    col_weights = col_weight.reshape(CBD, 1, BLOCK)
    first_blocks = lax.dynamic_slice(active_blocks, (device * RBD, 0), (RBD, 1)).reshape(-1)
    sent_points = call(
        spread_kernel, vmem_shape(N_COLS, PACKED, D, dtype=jnp.bfloat16), [SM, VM, VM]
    )(first_blocks, source_points, row_weights)
    points_here = exchange(sent_points, COLS)

    firsts = target_cluster.reshape(128, 128)[:, 0] - target_base
    target_means, target_logs = pl.pallas_call(
        target_means_kernel,
        out_shape=(vmem_shape(N_TGT, D), vmem_shape(1, N_TGT)),
        grid=(8,),
        in_specs=[
            SM,
            SM,
            pl.BlockSpec((2048, D), lambda k: (k, 0)),
            pl.BlockSpec((1, 1, 2048), lambda k: (k, 0, 0)),
        ],
        out_specs=(
            pl.BlockSpec((N_TGT, D), lambda k: (0, 0)),
            pl.BlockSpec((1, N_TGT), lambda k: (0, 0)),
        ),
        scratch_shapes=[pltpu.VMEM((N_TGT + PIECE, 2 * D), jnp.float32)],
        compiler_params=pltpu.CompilerParams(vmem_limit_bytes=24 << 20),
        cost_estimate=cost(1e9),
        name="target_means",
    )(target_base, firsts, in_hbm(target_points), in_hbm(target_cluster.reshape(8, 1, 2048)))

    group = lax.dynamic_slice_in_dim(active_blocks, row_index * N_COLS * RBD, N_COLS * RBD, 0)
    group_count = lax.dynamic_slice_in_dim(active_count, row_index * N_COLS * RBD, N_COLS * RBD)
    group_count = group_count.reshape(N_COLS, RBD)
    group = group.reshape(N_COLS, RBD, ACT)
    hit = group[:, :, 0] // CBD == col_index
    blocks = jnp.sum(jnp.where(hit[:, :, None], group % CBD, 0), axis=1).reshape(-1)
    counts = jnp.sum(jnp.where(hit, group_count, 0), axis=1)

    gains, source_logs, partial = call(
        coarse_start_kernel,
        (vmem_shape(N_SRC, N_TGT), vmem_shape(8, 128), vmem_shape(N_COLS, 8, 128)),
        [VM, VM],
        flops=1e9,
    )(in_vmem(gathered), in_vmem(target_means))
    gains, source_logs, target_logs = in_vmem(gains), in_vmem(source_logs), in_vmem(target_logs)

    def coarse_cols(parts, out_shape):
        return call(
            coarse_cols_kernel,
            out_shape,
            [VM] * (len(parts) + 2),
            [pltpu.VMEM((N_SRC, N_TGT), jnp.float32)],
        )(*[in_vmem(part) for part in parts], source_logs, gains)

    def coarse_rows(parts):
        return call(
            coarse_rows_kernel, vmem_shape(N_COLS, 8, 128), [VM] * (len(parts) + 2)
        )(*[in_vmem(part) for part in parts], target_logs, gains)

    for sweep in range(ITER_C):
        source_parts = [exchange(partial, COLS)]
        permuted = sweep in (0, ITER_C - 1)
        cols_shape = vmem_shape(1, N_TGT) if permuted else vmem_shape(N_ROWS, 1, N_TGT)
        cols_partial = coarse_cols(source_parts, cols_shape)
        if permuted:
            pair = lse_list([cols_partial, partner(cols_partial, "core", 1)])
            target_parts = four_along(pair, "x")
        else:
            target_parts = [exchange(cols_partial, ROWS)]
        if sweep + 1 < ITER_C:
            partial = coarse_rows(target_parts)

    slot_row = vmem_shape(N_COLS, 1, BLOCK)
    norms = pl.pallas_call(
        half_norms_kernel,
        out_shape=vmem_shape(CBD, 1, BLOCK),
        grid=(8,),
        in_specs=[pl.BlockSpec((2048, D), lambda k: (k, 0))],
        out_specs=pl.BlockSpec((8, 1, BLOCK), lambda k: (k, 0, 0)),
        compiler_params=pltpu.CompilerParams(vmem_limit_bytes=24 << 20),
        cost_estimate=cost(1e9),
        name="half_norms",
    )(in_hbm(target_points))
    fine_gains, halves, weights = call(
        products_kernel,
        (vmem_shape(N_COLS, BLOCK, WIDTH), slot_row, slot_row),
        [SM, SM, VM, ANY, ANY],
        [
            pltpu.VMEM((N_COLS, PACKED, D), jnp.bfloat16),
            pltpu.VMEM((N_COLS * ACT, BLOCK, D), jnp.bfloat16),
            pltpu.SemaphoreType.DMA((N_COLS, ACT + 1)),
        ],
        flops=1e9,
    )(counts, blocks, in_vmem(norms), in_hbm(points_here), in_hbm(target_points))
    fine_gains, halves, weights = in_vmem(fine_gains), in_vmem(halves), in_vmem(weights)
    column = vmem_shape(CBD, 1, BLOCK)
    values_scratch = pltpu.VMEM((CBD, 1, BLOCK), jnp.float32)
    work_scratch = pltpu.VMEM((BLOCK, WIDTH), jnp.float32)
    fine_shape = vmem_shape(N_COLS, BLOCK, WIDTH)
    best, fine_gains = call(
        first_pass_kernel,
        (column, fine_shape),
        [SM, SM, SM, SM, VM, VM, VM, VM, VM, VM],
        [values_scratch, pltpu.VMEM((N_TGT, 128), jnp.float32), work_scratch],
        input_output_aliases={9: 1},
    )(
        target_base,
        counts,
        blocks,
        firsts,
        *[in_vmem(part) for part in target_parts],
        target_cluster.reshape(CBD, 1, BLOCK),
        fine_gains,
    )
    best = lse_list([best, partner(best, "core", 1)])

    both, lam, fine_gains = call(
        second_pass_kernel,
        (vmem_shape(2 * CBD, 1, BLOCK), slot_row, fine_shape),
        [SM, SM, VM, VM, VM, VM, VM, VM],
        [values_scratch, work_scratch],
        input_output_aliases={7: 2},
    )(counts, blocks, *four_along_x(best), weights, in_vmem(fine_gains))
    other = partner(both, "core", 1)
    old, new = both[:CBD], other[:CBD]
    total = lse_list([old, new])
    mixed = both[CBD:] * jnp.exp2(old - total) + other[CBD:] * jnp.exp2(new - total)
    both = jnp.concatenate([total, mixed], axis=0)

    col_potential, col_adjoint, back = call(
        adjoint_kernel,
        (column, column, vmem_shape(N_COLS, 1, 2 * BLOCK)),
        [SM, SM, VM, VM, VM, VM, VM, VM, VM, VM, VM],
        [values_scratch],
    )(
        counts, blocks, *four_along_x(both), in_vmem(lam), halves, weights, col_weights,
        in_vmem(fine_gains),
    )
    back = exchange(back, COLS).reshape(N_COLS, 2 * BLOCK)
    chosen = (first_blocks // CBD)[:, None] == jnp.arange(N_COLS)[None, :]
    back = jnp.sum(jnp.where(chosen[:, :, None], back[None], 0.0), axis=1)
    return (
        back[:, :BLOCK].reshape(-1),
        col_potential.reshape(-1),
        back[:, BLOCK:].reshape(-1),
        col_adjoint.reshape(-1),
    )


def solution(mesh):
    split = Mesh(mesh.devices.reshape(4, 2, 4, 4), ALL)
    placed = (
        P(ALL, None),
        P(COLS, None),
        P(ALL),
        P(COLS),
        P(),
        P(),
        P(ALL),
        P(COLS),
    )
    return jax.shard_map(
        on_device,
        mesh=split,
        in_specs=placed,
        out_specs=(P(ALL), P(COLS), P(ALL), P(COLS)),
        check_vma=False,
    )
```

```python
import jax
import jax.numpy as jnp
from jax import lax
from jax.experimental import pallas as pl
from jax.experimental.pallas import tpu as pltpu
from jax.sharding import Mesh
from jax.sharding import PartitionSpec as P


D = 128
BLOCK = 256
ACT = 4
ITER_C = 4
CL_DEV = 64
RBD = 8
CBD = 64
ROWS = ("x", "core")
COLS = ("y", "z")
ALL = ("x", "core", "y", "z")
N_ROWS = 8
N_COLS = 16
N_SRC = CL_DEV * N_COLS
N_TGT = 512
PTS_SRC = 2048
PTS_TGT = 16384
PIECE = 32
TINY = 2.0**-80
PACKED = BLOCK + 16

SCALE = 2.8853900817779268
lowest = -1.0e30
HI = lax.Precision.HIGHEST
NT = (((1,), (1,)), ((), ()))

VM = pl.BlockSpec(memory_space=pltpu.VMEM)
SM = pl.BlockSpec(memory_space=pltpu.SMEM)
ANY = pl.BlockSpec(memory_space=pl.ANY)


def vmem_shape(*dims, dtype=jnp.float32):
    return pltpu.VMEM(dims, dtype)


def in_vmem(x):
    return pltpu.with_memory_space_constraint(x, pltpu.VMEM)


def shape(*dims):
    return pltpu.HBM(dims, jnp.float32)


def in_hbm(x):
    return pltpu.with_memory_space_constraint(x, pltpu.HBM)


def eye(rows, shift=0):
    return lax.broadcasted_iota(jnp.int32, (rows, 128), 0) + shift == lax.broadcasted_iota(
        jnp.int32, (rows, 128), 1
    )


def to_row(column, mask):
    return jnp.sum(jnp.where(mask, column, 0.0), axis=0, keepdims=True)


def to_column(row, mask):
    return jnp.sum(jnp.where(mask, row, 0.0), axis=1, keepdims=True)


def lse_list(parts):
    highest = parts[0]
    for part in parts[1:]:
        highest = jnp.maximum(highest, part)
    terms = [jnp.exp2(part - highest) for part in parts]
    while len(terms) > 1:
        terms = [terms[k] + terms[k + 1] for k in range(0, len(terms), 2)]
    return highest + jnp.log2(terms[0])


def one_hot(labels, rows):
    hit = lax.broadcasted_iota(jnp.int32, (rows, labels.shape[1]), 0) == labels
    return jnp.where(hit, 1.0, 0.0).astype(jnp.bfloat16)


def totals_and_counts(hits, points):
    both = jnp.concatenate([points, jnp.ones(points.shape, jnp.bfloat16)], axis=1)
    return jnp.dot(hits, both, preferred_element_type=jnp.float32)


def source_means_kernel(base, points, labels, out):
    both = totals_and_counts(one_hot(labels[...] - base[0], CL_DEV), points[...])
    counts = both[:, D:]
    means = both[:, :D] / counts
    low = to_row(counts, eye(CL_DEV))
    high = to_row(counts, eye(CL_DEV, 64))
    tail = lax.broadcasted_iota(jnp.int32, (8, 128), 0)
    tail = jnp.where(tail == 0, low, jnp.where(tail == 1, high, 0.0))
    for peer in range(N_COLS):
        out[peer, :CL_DEV, :] = means
        out[peer, CL_DEV:, :] = tail


def target_stats_kernel(base, firsts, labels, y_hbm, means, logs, norms, acc, ys, sems):
    copies = [
        pltpu.make_async_copy(
            y_hbm.at[k * 2048 : (k + 1) * 2048, :], ys.at[k * 2048 : (k + 1) * 2048, :], sems.at[k]
        )
        for k in range(8)
    ]
    for copy in copies:
        copy.start()
    acc[...] = jnp.zeros_like(acc)
    ones = jnp.full((8, 2 * D), 1.0, jnp.bfloat16)

    def piece(chunk, start, points_here):
        hits = one_hot(labels[chunk] - (start + base[0]), PIECE)
        window = pl.ds(pl.multiple_of(start, 8), PIECE)
        acc[window, :] += totals_and_counts(hits, points_here)

    for step in range(8):
        copies[step].wait()

        def some(n, most, step=step):
            for k in range(4):
                chunk = step * 8 + n * 4 + k
                points = ys[pl.ds(pl.multiple_of(chunk * BLOCK, BLOCK), BLOCK), :]
                start = firsts[2 * chunk] // 8 * 8
                piece(chunk, start, points)
                beyond = firsts[jnp.minimum(2 * chunk + 2, 127)]
                beyond = jnp.where(chunk < CBD - 1, beyond, N_TGT - 1)
                most = jnp.maximum(most, (beyond - start) // PIECE)
                wide = points.astype(jnp.float32)
                square = wide * wide
                high = square.astype(jnp.bfloat16)
                low = (square - high.astype(jnp.float32)).astype(jnp.bfloat16)
                both = jnp.concatenate([high, low], axis=1)
                total = lax.dot_general(ones, both, NT, preferred_element_type=jnp.float32)
                norms[chunk] = (0.5 * SCALE) * total[:1]
            return most

        most = lax.fori_loop(0, 2, some, 0)

        @pl.when(most > 0)
        def _(step=step):
            def chunk_rest(chunk, carry):
                start = firsts[2 * chunk] // 8 * 8
                beyond = firsts[jnp.minimum(2 * chunk + 2, 127)]
                beyond = jnp.where(chunk < CBD - 1, beyond, N_TGT - 1)

                def more(k, carry):
                    points = ys[pl.ds(pl.multiple_of(chunk * BLOCK, BLOCK), BLOCK), :]
                    piece(chunk, start + k * PIECE, points)
                    return carry

                lax.fori_loop(1, (beyond - start) // PIECE + 1, more, 0)
                return carry

            lax.fori_loop(step * 8, step * 8 + 8, chunk_rest, 0)

    mask = eye(128)
    for part in range(4):
        at = slice(part * 128, (part + 1) * 128)
        counts = acc[at, D:]
        means[at, :] = acc[at, :D] / counts
        logs[:, at] = jnp.log2(to_row(counts, mask))


def row_lse_chunk(scores):
    highest = jnp.max(scores, axis=1, keepdims=True)
    return highest + jnp.log2(jnp.sum(jnp.exp2(scores - highest), axis=1, keepdims=True))


def coarse_start_kernel(gathered, targets, gains, source_logs, out):
    mask = eye(128)
    y = targets[...]
    half_y = 0.5 * jnp.sum(y * y, axis=1, keepdims=True)
    half_y = jnp.concatenate(
        [to_row(half_y[k * 128 : (k + 1) * 128], mask) for k in range(4)], axis=1
    )
    for part in range(8):
        x = jnp.concatenate(
            [gathered[2 * part, :CL_DEV, :], gathered[2 * part + 1, :CL_DEV, :]], axis=0
        )
        counts = gathered[2 * part, 64:65, :] + gathered[2 * part + 1, 65:66, :]
        source_logs[part : part + 1, :] = jnp.log2(counts)
        half_x = 0.5 * jnp.sum(x * x, axis=1, keepdims=True)
        products = lax.dot_general(x, y, NT, precision=HI, preferred_element_type=jnp.float32)
        gain = SCALE * (products - (half_x + half_y))
        gains[part * 128 : (part + 1) * 128, :] = gain
        out[0, part : part + 1, :] = to_row(row_lse_chunk(gain), mask)
    first = out[0]
    for peer in range(1, N_COLS):
        out[peer] = first


def parts_of(refs):
    if len(refs) == 1:
        return [refs[0][k] for k in range(refs[0].shape[0])]
    return [ref[...] for ref in refs]


def coarse_rows_kernel(*refs):
    *gathered, target_logs, gains, out = refs
    mask = eye(128)
    potential = target_logs[...] - lse_list(parts_of(gathered))
    for part in range(8):
        pieces = []
        for piece in range(1):
            at = part * 128 + piece * 128
            pieces.append(row_lse_chunk(gains[at : at + 128, :] + potential))
        out[0, part : part + 1, :] = to_row(jnp.concatenate(pieces, axis=0), mask)
    first = out[0]
    for peer in range(1, N_COLS):
        out[peer] = first


def coarse_cols_kernel(*refs):
    *gathered, source_logs, gains, out, scores = refs
    mask = eye(128)
    potential = source_logs[...] - lse_list(parts_of(gathered))
    highest = jnp.full((8, N_TGT), lowest, jnp.float32)
    for part in range(8):
        at = slice(part * 128, (part + 1) * 128)
        value = gains[at, :] + to_column(potential[part : part + 1, :], mask)
        scores[at, :] = value
        highest = jnp.maximum(highest, jnp.max(value.reshape(16, 8, N_TGT), axis=0))
    highest = jnp.max(highest, axis=0, keepdims=True)
    total = jnp.zeros((8, N_TGT), jnp.float32)
    for part in range(8):
        at = slice(part * 128, (part + 1) * 128)
        value = jnp.exp2(scores[at, :] - highest)
        total = total + jnp.sum(value.reshape(16, 8, N_TGT), axis=0)
    result = highest + jnp.log2(jnp.sum(total, axis=0, keepdims=True))
    if len(out.shape) == 2:
        out[...] = result
    else:
        for peer in range(N_ROWS):
            out[peer] = result


def start_copies(counts, blocks, x_hbm, y_hbm, xs, ys, sems):
    def copies(slot):
        found = [pltpu.make_async_copy(x_hbm.at[slot], xs.at[slot], sems.at[slot, ACT])]
        for a in range(ACT):
            first = pl.multiple_of(blocks[slot * ACT + a] * BLOCK, BLOCK)
            found.append(
                pltpu.make_async_copy(
                    y_hbm.at[pl.ds(first, BLOCK), :], ys.at[slot * ACT + a], sems.at[slot, a]
                )
            )
        return found

    def begin(slot, carry):
        @pl.when(counts[slot] > 0)
        def _():
            for copy in copies(slot):
                copy.start()

        return carry

    lax.fori_loop(0, N_COLS, begin, 0)
    return copies


def products_kernel(counts, blocks, norms, x_hbm, y_hbm, gains, halves, weights, xs, ys, sems):
    copies = start_copies(counts, blocks, x_hbm, y_hbm, xs, ys, sems)
    mask = eye(128)

    def body(slot):
        x = xs[slot, :BLOCK, :]
        tail = xs[slot, BLOCK:, :].astype(jnp.float32)
        for h in range(2):
            at = slice(h * 128, (h + 1) * 128)
            wide = xs[slot, at, :].astype(jnp.float32)
            half_x = 0.5 * jnp.sum(wide * wide, axis=1, keepdims=True)
            halves[slot, :, at] = to_row(half_x, mask)
            weights[slot, :, at] = (tail[h : h + 1] + tail[h + 2 : h + 3]) + tail[h + 4 : h + 5]
        for a in range(ACT):
            products = lax.dot_general(
                x, ys[slot * ACT + a], NT, preferred_element_type=jnp.float32
            )
            gains[slot, :, a * BLOCK : (a + 1) * BLOCK] = (
                SCALE * products - norms[blocks[slot * ACT + a]]
            )

    each_slot(counts, body, copies)


def slot_potential(slot, counts, blocks, values):
    rows = []
    for a in range(ACT):
        row = values[blocks[slot * ACT + a]]
        rows.append(jnp.where(a < counts[slot], row, lowest))
    return jnp.concatenate(rows, axis=1)


CHUNK = 8
CHUNKS = BLOCK // CHUNK
WIDTH = ACT * BLOCK


def merge_columns(slot, counts, blocks, values, best, mixed, result, mean):
    for a in range(ACT):
        block = blocks[slot * ACT + a]
        at = slice(a * BLOCK, (a + 1) * BLOCK)
        here = jnp.where(a < counts[slot], result[:, at] - values[block], lowest)
        old = best[block]
        top = jnp.maximum(old, here)
        old_part, new_part = jnp.exp2(old - top), jnp.exp2(here - top)
        both = old_part + new_part
        best[block] = top + jnp.log2(both)
        if mean is not None:
            part = jnp.where(a < counts[slot], mean[:, at], 0.0)
            mixed[block] = (mixed[block] * old_part + part * new_part) / both


GROUP = 256
FAST = 8


def fast_slot(slot, counts, blocks, gains, values, best, least, sums, cols, weights=None, mixed=None, lam_out=None):
    potential = slot_potential(slot, counts, blocks, values)
    mask = eye(128)
    if weights is not None:
        w_row = weights[slot]
        for h in range(2):
            at = slice(h * 128, (h + 1) * 128)
            cols[at, 0:1] = to_column(w_row[:, at], mask)
    sums[...] = jnp.zeros(sums.shape, jnp.float32)

    def group(step, carry):
        total = sums[:8, :]
        weighted = sums[8:, :]
        for k in range(GROUP // FAST):
            at = pl.ds(pl.multiple_of(step * GROUP + k * FAST, FAST), FAST)
            scores = gains[slot, at, :] + potential
            highest = jnp.max(scores, axis=1, keepdims=True)
            entries = jnp.exp2(scores - highest)
            mass = jnp.sum(entries, axis=1, keepdims=True)
            if lam_out is not None:
                cols[at, 1:2] = highest + jnp.log2(mass)
            scale = 1.0 / mass
            part = (entries * scale).reshape(FAST // 8, 8, WIDTH)
            total = total + jnp.sum(part, axis=0)
            if weights is not None:
                part = (entries * (scale * cols[at, 0:1])).reshape(FAST // 8, 8, WIDTH)
                weighted = weighted + jnp.sum(part, axis=0)
        sums[:8, :] = total
        if weights is not None:
            sums[8:, :] = weighted
        return carry

    lax.fori_loop(0, BLOCK // GROUP, group, 0)
    total = jnp.sum(sums[:8, :], axis=0, keepdims=True)
    mean = None if weights is None else jnp.sum(sums[8:, :], axis=0, keepdims=True) / total
    for a in range(ACT):
        part = jnp.where(a < counts[slot], total[:, a * BLOCK : (a + 1) * BLOCK], 1.0)
        least[...] = jnp.minimum(least[...], part)
    merge_columns(slot, counts, blocks, values, best, mixed, jnp.log2(total), mean)
    if lam_out is not None:
        for h in range(2):
            at = slice(h * 128, (h + 1) * 128)
            lam_out[slot, :, at] = to_row(cols[at, 1:2], mask)


def fine_pass(counts, blocks, gains, work, values, best, least, sums, cols, weights=None, mixed=None, lam_out=None):
    clear(best, mixed)
    least[...] = jnp.ones(least.shape, jnp.float32)
    each_slot(
        counts,
        lambda slot: fast_slot(
            slot, counts, blocks, gains, values, best, least, sums, cols, weights, mixed, lam_out
        ),
    )

    @pl.when(jnp.logical_not(jnp.min(least[...]) > TINY))
    def _():
        clear(best, mixed)
        each_slot(
            counts,
            lambda slot: fine_slot(
                slot, counts, blocks, gains, work, values, best, weights, mixed, lam_out
            ),
        )


def fine_slot(slot, counts, blocks, gains, work, values, best, weights=None, mixed=None, lam_out=None):
    potential = slot_potential(slot, counts, blocks, values)
    mask = eye(128)
    highest = jnp.full((8, WIDTH), lowest, jnp.float32)
    lams = []
    for k in range(CHUNKS):
        at = slice(k * CHUNK, (k + 1) * CHUNK)
        scores = gains[slot, at, :] + potential
        lam = row_lse_chunk(scores)
        scores = scores - lam
        work[at, :] = scores
        highest = jnp.maximum(highest, jnp.max(scores.reshape(CHUNK // 8, 8, WIDTH), axis=0))
        lams.append(lam)
    highest = jnp.max(highest, axis=0, keepdims=True)
    total = jnp.zeros((8, WIDTH), jnp.float32)
    if weights is not None:
        w_row = weights[slot]
        w_cols = [to_column(w_row[:, h * 128 : (h + 1) * 128], mask) for h in range(2)]
        w_col = jnp.concatenate(w_cols, axis=0)
        weighted = jnp.zeros((8, WIDTH), jnp.float32)
    for k in range(CHUNKS):
        at = slice(k * CHUNK, (k + 1) * CHUNK)
        value = jnp.exp2(work[at, :] - highest)
        total = total + jnp.sum(value.reshape(CHUNK // 8, 8, WIDTH), axis=0)
        if weights is not None:
            value = value * w_col[at]
            weighted = weighted + jnp.sum(value.reshape(CHUNK // 8, 8, WIDTH), axis=0)
    total = jnp.sum(total, axis=0, keepdims=True)
    result = highest + jnp.log2(total)
    mean = None if weights is None else jnp.sum(weighted, axis=0, keepdims=True) / total
    merge_columns(slot, counts, blocks, values, best, mixed, result, mean)
    if lam_out is not None:
        for h in range(2):
            at = slice(h * 128, (h + 1) * 128)
            lam_out[slot, :, at] = to_row(jnp.concatenate(lams[h * CHUNKS // 2 : (h + 1) * CHUNKS // 2], axis=0), mask)


def clear(best, mixed=None):
    best[...] = jnp.full(best.shape, lowest, jnp.float32)
    if mixed is not None:
        mixed[...] = jnp.zeros(mixed.shape, jnp.float32)


def each_slot(counts, body, copies=None):
    def step(slot, carry):
        @pl.when(counts[slot] > 0)
        def _():
            if copies is not None:
                for copy in copies(slot):
                    copy.wait()
            body(slot)

        return carry

    lax.fori_loop(0, N_COLS, step, 0)


def first_pass_kernel(
    base, counts, blocks, p0, p1, p2, p3, labels, gains, best, kept, values, work, least, sums, cols
):
    cluster_values = -lse_list([p0[...], p1[...], p2[...], p3[...]])
    index = labels[...] - base[0]
    found = jnp.zeros((128, 128), jnp.float32)
    for part in range(4):
        row = cluster_values[:, part * 128 : (part + 1) * 128]
        picked = jnp.take_along_axis(
            jnp.broadcast_to(row, (128, 128)), index & 127, axis=1, mode="promise_in_bounds"
        )
        found = jnp.where(index >> 7 == part, picked, found)
    for chunk in range(128):
        at = slice(chunk % 2 * 128, (chunk % 2 + 1) * 128)
        values[chunk // 2, :, at] = found[chunk : chunk + 1, :]
    fine_pass(counts, blocks, gains, work, values, best, least, sums, cols)


def second_pass_kernel(
    counts, blocks, l0, l1, l2, l3, weights, gains, best, mixed, lam, kept, values, work, least, sums, cols
):
    values[...] = -lse_list([l0[...], l1[...], l2[...], l3[...]])
    fine_pass(counts, blocks, gains, work, values, best, least, sums, cols, weights, mixed, lam)


def adjoint_kernel(
    counts, blocks, l0, l1, l2, l3, lam, halves, weights, col_weights, gains,
    potential_out, back, values,
):
    total = lse_list([l0[...], l1[...], l2[...], l3[...]])
    values[...] = -total
    potential_out[...] = total * (-1.0 / SCALE)
    back[...] = jnp.zeros(back.shape, jnp.float32)
    mask = eye(128)

    def body(slot):
        potential = slot_potential(slot, counts, blocks, values)
        spread = jnp.concatenate(
            [col_weights[blocks[slot * ACT + a]] for a in range(ACT)], axis=1
        )
        for h in range(2):
            half = slice(h * 128, (h + 1) * 128)
            shift = to_column(lam[slot, :, half], mask)
            sums, crossed = [], []
            for k in range(128 // CHUNK):
                at = slice(h * 128 + k * CHUNK, h * 128 + (k + 1) * CHUNK)
                scores = gains[slot, at, :] + potential
                entries = jnp.exp2(scores - shift[k * CHUNK : (k + 1) * CHUNK])
                sums.append(jnp.sum(entries, axis=1, keepdims=True))
                crossed.append(jnp.sum(entries * spread, axis=1, keepdims=True))
            mass = to_row(jnp.concatenate(sums, axis=0), mask)
            cross = to_row(jnp.concatenate(crossed, axis=0), mask)
            back[slot, :, half] = halves[slot, :, half] - lam[slot, :, half] * (1.0 / SCALE)
            back[slot, :, BLOCK + h * 128 : BLOCK + (h + 1) * 128] = (
                weights[slot, :, half] * mass + cross
            )

    each_slot(counts, body)


def plan_kernel(row, col, lists_hbm, counts_hbm, counts, blocks, owners, lists, found, sems):
    first = pl.multiple_of(row[0] * 128, 128)
    copies = [
        pltpu.make_async_copy(lists_hbm.at[:, pl.ds(first, 128)], lists, sems.at[0]),
        pltpu.make_async_copy(counts_hbm.at[row[0]], found, sems.at[1]),
    ]
    for copy in copies:
        copy.start()
    for copy in copies:
        copy.wait()
    for q in range(RBD):
        owners[q] = lists[0, col[0] * RBD + q] >> 6

    def fill(slot, carry):
        count = jnp.int32(0)
        chosen = [jnp.int32(0)] * ACT
        for q in range(RBD):
            index = slot * RBD + q
            here = (lists[0, index] >> 6) == col[0]
            count = jnp.where(here, found[index], count)
            chosen = [
                jnp.where(here, lists[a, index] & (CBD - 1), old) for a, old in enumerate(chosen)
            ]
        counts[slot] = count
        for a in range(ACT):
            blocks[slot * ACT + a] = chosen[a]
        return carry

    lax.fori_loop(0, N_COLS, fill, 0)


def home_kernel(owners, back, potential, adjoint):
    for q in range(RBD):
        got = back[owners[q]]
        for h in range(2):
            at = slice(2 * q + h, 2 * q + h + 1)
            potential[at, :] = got[:, h * 128 : (h + 1) * 128]
            adjoint[at, :] = got[:, BLOCK + h * 128 : BLOCK + (h + 1) * 128]


def spread_kernel(owners, points, weights, out):
    for q in range(RBD):
        owner = owners[q]
        out[owner, :BLOCK, :] = points[q * BLOCK : (q + 1) * BLOCK, :]
        rest = weights[q]
        pieces = []
        for _ in range(3):
            piece = rest.astype(jnp.bfloat16)
            rest = rest - piece.astype(jnp.float32)
            pieces.append(piece.astype(jnp.float32))
        pieces.append(jnp.zeros((10, D), jnp.float32))
        out[owner, BLOCK:, :] = jnp.concatenate(pieces, axis=0).astype(jnp.bfloat16)


def cost(flops):
    return pl.CostEstimate(flops=int(flops), transcendentals=0, bytes_accessed=4 << 20)


def call(kernel, out_shape, in_specs, scratch=(), flops=1e8, **kw):
    out_specs = jax.tree.map(lambda _: VM, out_shape, is_leaf=lambda x: hasattr(x, "shape"))
    return pl.pallas_call(
        kernel,
        out_shape=out_shape,
        in_specs=in_specs,
        out_specs=out_specs,
        scratch_shapes=list(scratch),
        compiler_params=pltpu.CompilerParams(vmem_limit_bytes=24 << 20),
        cost_estimate=cost(flops),
        **kw,
    )


def exchange(x, axis):
    return lax.all_to_all(x, axis, split_axis=0, concat_axis=0, tiled=True)


def partner(x, axis, step):
    n = lax.axis_size(axis)
    return lax.ppermute(x, axis, [(k, k ^ step) for k in range(n)])


def four_along(x, axis):
    found = [x]
    for step in (1, 2, 3):
        found.append(partner(x, axis, step))
    return found


def four_along_x(x):
    return [in_vmem(part) for part in four_along(x, "x")]


def on_device(
    source_points,
    target_points,
    source_cluster,
    target_cluster,
    active_blocks,
    active_count,
    row_weight,
    col_weight,
):
    row_index = lax.axis_index(ROWS)
    col_index = lax.axis_index(COLS)
    device = row_index * N_COLS + col_index

    source_base = (CL_DEV * device).reshape(1).astype(jnp.int32)
    target_base = (N_TGT * col_index).reshape(1).astype(jnp.int32)
    packed = call(
        source_means_kernel, vmem_shape(N_COLS, CL_DEV + 8, D), [SM, VM, VM]
    )(source_base, in_hbm(source_points), in_hbm(source_cluster.reshape(1, PTS_SRC)))
    gathered = exchange(packed, COLS)

    row_weights = row_weight.reshape(RBD, 2, 128)
    col_weights = col_weight.reshape(CBD, 1, BLOCK)
    counts, blocks, owners = pl.pallas_call(
        plan_kernel,
        out_shape=tuple(jax.ShapeDtypeStruct((n,), jnp.int32) for n in (N_COLS, N_COLS * ACT, RBD)),
        in_specs=[SM, SM, ANY, ANY],
        out_specs=(SM, SM, SM),
        scratch_shapes=[
            pltpu.SMEM((ACT, 128), jnp.int32),
            pltpu.SMEM((128,), jnp.int32),
            pltpu.SemaphoreType.DMA((2,)),
        ],
        name="plan",
    )(
        row_index.reshape(1).astype(jnp.int32),
        col_index.reshape(1).astype(jnp.int32),
        in_hbm(active_blocks.T),
        in_hbm(active_count.reshape(8, 128)),
    )
    sent_points = call(
        spread_kernel, vmem_shape(N_COLS, PACKED, D, dtype=jnp.bfloat16), [SM, VM, VM]
    )(owners, in_hbm(source_points), in_hbm(row_weights))
    points_here = exchange(sent_points, COLS)

    firsts = target_cluster.reshape(128, 128)[:, 0] - target_base
    target_means, target_logs, norms = call(
        target_stats_kernel,
        (vmem_shape(N_TGT, D), vmem_shape(1, N_TGT), vmem_shape(CBD, 1, BLOCK)),
        [SM, SM, VM, ANY],
        [
            pltpu.VMEM((N_TGT + PIECE, 2 * D), jnp.float32),
            pltpu.VMEM((PTS_TGT, D), jnp.bfloat16),
            pltpu.SemaphoreType.DMA((8,)),
        ],
        flops=1e9,
    )(target_base, firsts, target_cluster.reshape(CBD, 1, BLOCK), in_hbm(target_points))

    gains, source_logs, partial = call(
        coarse_start_kernel,
        (vmem_shape(N_SRC, N_TGT), vmem_shape(8, 128), vmem_shape(N_COLS, 8, 128)),
        [VM, VM],
        flops=1e9,
    )(in_vmem(gathered), in_vmem(target_means))
    gains, source_logs, target_logs = in_vmem(gains), in_vmem(source_logs), in_vmem(target_logs)

    def coarse_cols(parts, out_shape):
        return call(
            coarse_cols_kernel,
            out_shape,
            [VM] * (len(parts) + 2),
            [pltpu.VMEM((N_SRC, N_TGT), jnp.float32)],
        )(*[in_vmem(part) for part in parts], source_logs, gains)

    def coarse_rows(parts):
        return call(
            coarse_rows_kernel, vmem_shape(N_COLS, 8, 128), [VM] * (len(parts) + 2)
        )(*[in_vmem(part) for part in parts], target_logs, gains)

    for sweep in range(ITER_C):
        source_parts = [exchange(partial, COLS)]
        permuted = sweep in (0, ITER_C - 1)
        cols_shape = vmem_shape(1, N_TGT) if permuted else vmem_shape(N_ROWS, 1, N_TGT)
        cols_partial = coarse_cols(source_parts, cols_shape)
        if permuted:
            pair = lse_list([cols_partial, partner(cols_partial, "core", 1)])
            target_parts = four_along(pair, "x")
        else:
            target_parts = [exchange(cols_partial, ROWS)]
        if sweep + 1 < ITER_C:
            partial = coarse_rows(target_parts)

    slot_row = vmem_shape(N_COLS, 1, BLOCK)
    fine_gains, halves, weights = call(
        products_kernel,
        (vmem_shape(N_COLS, BLOCK, WIDTH), slot_row, slot_row),
        [SM, SM, VM, ANY, ANY],
        [
            pltpu.VMEM((N_COLS, PACKED, D), jnp.bfloat16),
            pltpu.VMEM((N_COLS * ACT, BLOCK, D), jnp.bfloat16),
            pltpu.SemaphoreType.DMA((N_COLS, ACT + 1)),
        ],
        flops=1e9,
    )(counts, blocks, in_vmem(norms), in_hbm(points_here), in_hbm(target_points))
    fine_gains, halves, weights = in_vmem(fine_gains), in_vmem(halves), in_vmem(weights)
    column = vmem_shape(CBD, 1, BLOCK)
    values_scratch = pltpu.VMEM((CBD, 1, BLOCK), jnp.float32)
    work_scratch = pltpu.VMEM((BLOCK, WIDTH), jnp.float32)
    fast_scratch = [
        pltpu.VMEM((1, BLOCK), jnp.float32),
        pltpu.VMEM((16, WIDTH), jnp.float32),
        pltpu.VMEM((BLOCK, 8), jnp.float32),
    ]
    fine_shape = vmem_shape(N_COLS, BLOCK, WIDTH)
    best, fine_gains = call(
        first_pass_kernel,
        (column, fine_shape),
        [SM, SM, SM, VM, VM, VM, VM, VM, VM],
        [values_scratch, work_scratch, *fast_scratch],
        input_output_aliases={8: 1},
    )(
        target_base,
        counts,
        blocks,
        *[in_vmem(part) for part in target_parts],
        target_cluster.reshape(128, 128),
        fine_gains,
    )
    best = lse_list([best, partner(best, "core", 1)])

    best, mixed, lam, fine_gains = call(
        second_pass_kernel,
        (column, column, slot_row, fine_shape),
        [SM, SM, VM, VM, VM, VM, VM, VM],
        [values_scratch, work_scratch, *fast_scratch],
        input_output_aliases={7: 3},
    )(counts, blocks, *four_along_x(best), weights, in_vmem(fine_gains))
    other = partner(best, "core", 1)
    other_mixed = partner(mixed, "core", 1)
    total = lse_list([best, other])
    mixed = mixed * jnp.exp2(best - total) + other_mixed * jnp.exp2(other - total)
    best_parts = four_along(total, "x")
    mixed_parts = four_along(mixed, "x")

    col_potential, back = call(
        adjoint_kernel,
        (shape(CBD, 1, BLOCK), vmem_shape(N_COLS, 1, 2 * BLOCK)),
        [SM, SM, VM, VM, VM, VM, VM, VM, VM, VM, VM],
        [values_scratch],
    )(
        counts, blocks, *[in_vmem(part) for part in best_parts], in_vmem(lam), halves,
        weights, col_weights, in_vmem(fine_gains),
    )
    total = lse_list(best_parts)
    mixed = [m * jnp.exp2(part - total) for m, part in zip(mixed_parts, best_parts)]
    col_adjoint = ((mixed[0] + mixed[1]) + (mixed[2] + mixed[3])) + col_weights
    back = exchange(back, COLS)
    row_potential, row_adjoint = call(
        home_kernel, (shape(16, 128), shape(16, 128)), [SM, VM]
    )(owners, in_vmem(back))
    return (
        row_potential.reshape(-1),
        col_potential.reshape(-1),
        row_adjoint.reshape(-1),
        col_adjoint.reshape(-1),
    )


def solution(mesh):
    split = Mesh(mesh.devices.reshape(4, 2, 4, 4), ALL)
    placed = (
        P(ALL, None),
        P(COLS, None),
        P(ALL),
        P(COLS),
        P(),
        P(),
        P(ALL),
        P(COLS),
    )
    return jax.shard_map(
        on_device,
        mesh=split,
        in_specs=placed,
        out_specs=(P(ALL), P(COLS), P(ALL), P(COLS)),
        check_vma=False,
    )
```

```python
import jax
import jax.numpy as jnp
from jax import lax
from jax.experimental import pallas as pl
from jax.experimental.pallas import tpu as pltpu
from jax.sharding import Mesh
from jax.sharding import PartitionSpec as P


D = 128
BLOCK = 256
ACT = 4
ITER_C = 4
CL_DEV = 64
RBD = 8
CBD = 64
ROWS = ("x", "core")
COLS = ("y", "z")
ALL = ("x", "core", "y", "z")
N_ROWS = 8
N_COLS = 16
N_SRC = CL_DEV * N_COLS
N_TGT = 512
PTS_SRC = 2048
PTS_TGT = 16384
PIECE = 32
TINY = 2.0**-80
PACKED = BLOCK + 16

SCALE = 2.8853900817779268
lowest = -1.0e30
HI = lax.Precision.HIGHEST
NT = (((1,), (1,)), ((), ()))

VM = pl.BlockSpec(memory_space=pltpu.VMEM)
SM = pl.BlockSpec(memory_space=pltpu.SMEM)
ANY = pl.BlockSpec(memory_space=pl.ANY)


def vmem_shape(*dims, dtype=jnp.float32):
    return pltpu.VMEM(dims, dtype)


def in_vmem(x):
    return pltpu.with_memory_space_constraint(x, pltpu.VMEM)


def shape(*dims):
    return pltpu.HBM(dims, jnp.float32)


def in_hbm(x):
    return pltpu.with_memory_space_constraint(x, pltpu.HBM)


def eye(rows, shift=0):
    return lax.broadcasted_iota(jnp.int32, (rows, 128), 0) + shift == lax.broadcasted_iota(
        jnp.int32, (rows, 128), 1
    )


def to_row(column, mask):
    return jnp.sum(jnp.where(mask, column, 0.0), axis=0, keepdims=True)


def to_column(row, mask):
    return jnp.sum(jnp.where(mask, row, 0.0), axis=1, keepdims=True)


def lse_list(parts):
    highest = parts[0]
    for part in parts[1:]:
        highest = jnp.maximum(highest, part)
    terms = [jnp.exp2(part - highest) for part in parts]
    while len(terms) > 1:
        terms = [terms[k] + terms[k + 1] for k in range(0, len(terms), 2)]
    return highest + jnp.log2(terms[0])


def one_hot(labels, rows):
    hit = lax.broadcasted_iota(jnp.int32, (rows, labels.shape[1]), 0) == labels
    return jnp.where(hit, 1.0, 0.0).astype(jnp.bfloat16)


def totals_and_counts(hits, points):
    both = jnp.concatenate([points, jnp.ones(points.shape, jnp.bfloat16)], axis=1)
    return jnp.dot(hits, both, preferred_element_type=jnp.float32)


def square_sums(points, factor):
    wide = points.astype(jnp.float32)
    square = wide * wide
    high = square.astype(jnp.bfloat16)
    low = (square - high.astype(jnp.float32)).astype(jnp.bfloat16)
    ones = jnp.full((8, 2 * D), 1.0, jnp.bfloat16)
    both = jnp.concatenate([high, low], axis=1)
    return factor * lax.dot_general(ones, both, NT, preferred_element_type=jnp.float32)[:1]


def source_means_kernel(base, points, labels, out):
    both = totals_and_counts(one_hot(labels[...] - base[0], CL_DEV), points[...])
    counts = both[:, D:]
    means = both[:, :D] / counts
    low = to_row(counts, eye(CL_DEV))
    high = to_row(counts, eye(CL_DEV, 64))
    tail = lax.broadcasted_iota(jnp.int32, (8, 128), 0)
    tail = jnp.where(tail == 0, low, jnp.where(tail == 1, high, 0.0))
    for peer in range(N_COLS):
        out[peer, :CL_DEV, :] = means
        out[peer, CL_DEV:, :] = tail


def target_stats_kernel(base, firsts, labels, y_hbm, means, logs, norms, acc, ys, sems):
    copies = [
        pltpu.make_async_copy(
            y_hbm.at[k * 2048 : (k + 1) * 2048, :], ys.at[k * 2048 : (k + 1) * 2048, :], sems.at[k]
        )
        for k in range(8)
    ]
    for copy in copies:
        copy.start()
    acc[...] = jnp.zeros_like(acc)

    def piece(chunk, start, points_here):
        hits = one_hot(labels[chunk] - (start + base[0]), PIECE)
        window = pl.ds(pl.multiple_of(start, 8), PIECE)
        acc[window, :] += totals_and_counts(hits, points_here)

    for step in range(8):
        copies[step].wait()

        def some(n, most, step=step):
            for k in range(4):
                chunk = step * 8 + n * 4 + k
                points = ys[pl.ds(pl.multiple_of(chunk * BLOCK, BLOCK), BLOCK), :]
                start = firsts[2 * chunk] // 8 * 8
                piece(chunk, start, points)
                beyond = firsts[jnp.minimum(2 * chunk + 2, 127)]
                beyond = jnp.where(chunk < CBD - 1, beyond, N_TGT - 1)
                most = jnp.maximum(most, (beyond - start) // PIECE)
                norms[chunk] = square_sums(points, 0.5 * SCALE)
            return most

        most = lax.fori_loop(0, 2, some, 0)

        @pl.when(most > 0)
        def _(step=step):
            def chunk_rest(chunk, carry):
                start = firsts[2 * chunk] // 8 * 8
                beyond = firsts[jnp.minimum(2 * chunk + 2, 127)]
                beyond = jnp.where(chunk < CBD - 1, beyond, N_TGT - 1)

                def more(k, carry):
                    points = ys[pl.ds(pl.multiple_of(chunk * BLOCK, BLOCK), BLOCK), :]
                    piece(chunk, start + k * PIECE, points)
                    return carry

                lax.fori_loop(1, (beyond - start) // PIECE + 1, more, 0)
                return carry

            lax.fori_loop(step * 8, step * 8 + 8, chunk_rest, 0)

    mask = eye(128)
    for part in range(4):
        at = slice(part * 128, (part + 1) * 128)
        counts = acc[at, D:]
        means[at, :] = acc[at, :D] / counts
        logs[:, at] = jnp.log2(to_row(counts, mask))


def row_lse_chunk(scores):
    highest = jnp.max(scores, axis=1, keepdims=True)
    return highest + jnp.log2(jnp.sum(jnp.exp2(scores - highest), axis=1, keepdims=True))


def coarse_start_kernel(gathered, targets, gains, source_logs, out):
    mask = eye(128)
    y = targets[...]
    half_y = 0.5 * jnp.sum(y * y, axis=1, keepdims=True)
    half_y = jnp.concatenate(
        [to_row(half_y[k * 128 : (k + 1) * 128], mask) for k in range(4)], axis=1
    )
    for part in range(8):
        x = jnp.concatenate(
            [gathered[2 * part, :CL_DEV, :], gathered[2 * part + 1, :CL_DEV, :]], axis=0
        )
        counts = gathered[2 * part, 64:65, :] + gathered[2 * part + 1, 65:66, :]
        source_logs[part : part + 1, :] = jnp.log2(counts)
        half_x = 0.5 * jnp.sum(x * x, axis=1, keepdims=True)
        products = lax.dot_general(x, y, NT, precision=HI, preferred_element_type=jnp.float32)
        gain = SCALE * (products - (half_x + half_y))
        gains[part * 128 : (part + 1) * 128, :] = gain
        out[0, part : part + 1, :] = to_row(row_lse_chunk(gain), mask)
    first = out[0]
    for peer in range(1, N_COLS):
        out[peer] = first


def parts_of(refs):
    if len(refs) == 1:
        return [refs[0][k] for k in range(refs[0].shape[0])]
    return [ref[...] for ref in refs]


def coarse_rows_kernel(*refs):
    *gathered, target_logs, gains, out = refs
    mask = eye(128)
    potential = target_logs[...] - lse_list(parts_of(gathered))
    for part in range(8):
        pieces = []
        for piece in range(1):
            at = part * 128 + piece * 128
            pieces.append(row_lse_chunk(gains[at : at + 128, :] + potential))
        out[0, part : part + 1, :] = to_row(jnp.concatenate(pieces, axis=0), mask)
    first = out[0]
    for peer in range(1, N_COLS):
        out[peer] = first


def coarse_cols_kernel(*refs):
    *gathered, source_logs, gains, out, scores = refs
    mask = eye(128)
    potential = source_logs[...] - lse_list(parts_of(gathered))
    highest = jnp.full((8, N_TGT), lowest, jnp.float32)
    for part in range(8):
        at = slice(part * 128, (part + 1) * 128)
        value = gains[at, :] + to_column(potential[part : part + 1, :], mask)
        scores[at, :] = value
        highest = jnp.maximum(highest, jnp.max(value.reshape(16, 8, N_TGT), axis=0))
    highest = jnp.max(highest, axis=0, keepdims=True)
    total = jnp.zeros((8, N_TGT), jnp.float32)
    for part in range(8):
        at = slice(part * 128, (part + 1) * 128)
        value = jnp.exp2(scores[at, :] - highest)
        total = total + jnp.sum(value.reshape(16, 8, N_TGT), axis=0)
    result = highest + jnp.log2(jnp.sum(total, axis=0, keepdims=True))
    if len(out.shape) == 2:
        out[...] = result
    else:
        for peer in range(N_ROWS):
            out[peer] = result


def start_copies(counts, blocks, x_hbm, y_hbm, xs, ys, sems):
    def copies(slot):
        found = [pltpu.make_async_copy(x_hbm.at[slot], xs.at[slot], sems.at[slot, ACT])]
        for a in range(ACT):
            first = pl.multiple_of(blocks[slot * ACT + a] * BLOCK, BLOCK)
            found.append(
                pltpu.make_async_copy(
                    y_hbm.at[pl.ds(first, BLOCK), :], ys.at[slot * ACT + a], sems.at[slot, a]
                )
            )
        return found

    def begin(slot, carry):
        @pl.when(counts[slot] > 0)
        def _():
            for copy in copies(slot):
                copy.start()

        return carry

    lax.fori_loop(0, N_COLS, begin, 0)
    return copies


def products_kernel(counts, blocks, norms, x_hbm, y_hbm, gains, halves, weights, xs, ys, sems):
    copies = start_copies(counts, blocks, x_hbm, y_hbm, xs, ys, sems)

    def body(slot):
        x = xs[slot, :BLOCK, :]
        tail = xs[slot, BLOCK:, :].astype(jnp.float32)
        halves[slot] = square_sums(x, 0.5)
        for h in range(2):
            at = slice(h * 128, (h + 1) * 128)
            weights[slot, :, at] = (tail[h : h + 1] + tail[h + 2 : h + 3]) + tail[h + 4 : h + 5]
        for a in range(ACT):
            products = lax.dot_general(
                x, ys[slot * ACT + a], NT, preferred_element_type=jnp.float32
            )
            gains[slot, :, a * BLOCK : (a + 1) * BLOCK] = (
                SCALE * products - norms[blocks[slot * ACT + a]]
            )

    each_slot(counts, body, copies)


def slot_potential(slot, counts, blocks, values):
    rows = []
    for a in range(ACT):
        row = values[blocks[slot * ACT + a]]
        rows.append(jnp.where(a < counts[slot], row, lowest))
    return jnp.concatenate(rows, axis=1)


CHUNK = 8
CHUNKS = BLOCK // CHUNK
WIDTH = ACT * BLOCK


def merge_columns(slot, counts, blocks, values, best, mixed, result, mean):
    for a in range(ACT):
        block = blocks[slot * ACT + a]
        at = slice(a * BLOCK, (a + 1) * BLOCK)
        here = jnp.where(a < counts[slot], result[:, at] - values[block], lowest)
        old = best[block]
        top = jnp.maximum(old, here)
        old_part, new_part = jnp.exp2(old - top), jnp.exp2(here - top)
        both = old_part + new_part
        best[block] = top + jnp.log2(both)
        if mean is not None:
            part = jnp.where(a < counts[slot], mean[:, at], 0.0)
            mixed[block] = (mixed[block] * old_part + part * new_part) / both


GROUP = 256
FAST = 8


def fast_slot(slot, counts, blocks, gains, values, best, least, sums, cols, weights=None, mixed=None, lam_out=None):
    potential = slot_potential(slot, counts, blocks, values)
    mask = eye(128)
    if weights is not None:
        w_row = weights[slot]
        for h in range(2):
            at = slice(h * 128, (h + 1) * 128)
            cols[at, 0:1] = to_column(w_row[:, at], mask)
    sums[...] = jnp.zeros(sums.shape, jnp.float32)

    def group(step, carry):
        total = sums[:8, :]
        weighted = sums[8:, :]
        for k in range(GROUP // FAST):
            at = pl.ds(pl.multiple_of(step * GROUP + k * FAST, FAST), FAST)
            scores = gains[slot, at, :] + potential
            highest = jnp.max(scores, axis=1, keepdims=True)
            entries = jnp.exp2(scores - highest)
            mass = jnp.sum(entries, axis=1, keepdims=True)
            if lam_out is not None:
                cols[at, 1:2] = highest + jnp.log2(mass)
            scale = 1.0 / mass
            part = (entries * scale).reshape(FAST // 8, 8, WIDTH)
            total = total + jnp.sum(part, axis=0)
            if weights is not None:
                part = (entries * (scale * cols[at, 0:1])).reshape(FAST // 8, 8, WIDTH)
                weighted = weighted + jnp.sum(part, axis=0)
        sums[:8, :] = total
        if weights is not None:
            sums[8:, :] = weighted
        return carry

    lax.fori_loop(0, BLOCK // GROUP, group, 0)
    total = jnp.sum(sums[:8, :], axis=0, keepdims=True)
    mean = None if weights is None else jnp.sum(sums[8:, :], axis=0, keepdims=True) / total
    for a in range(ACT):
        part = jnp.where(a < counts[slot], total[:, a * BLOCK : (a + 1) * BLOCK], 1.0)
        least[...] = jnp.minimum(least[...], part)
    merge_columns(slot, counts, blocks, values, best, mixed, jnp.log2(total), mean)
    if lam_out is not None:
        for h in range(2):
            at = slice(h * 128, (h + 1) * 128)
            lam_out[slot, :, at] = to_row(cols[at, 1:2], mask)


def fine_pass(counts, blocks, gains, work, values, best, least, sums, cols, weights=None, mixed=None, lam_out=None):
    clear(best, mixed)
    least[...] = jnp.ones(least.shape, jnp.float32)
    each_slot(
        counts,
        lambda slot: fast_slot(
            slot, counts, blocks, gains, values, best, least, sums, cols, weights, mixed, lam_out
        ),
    )

    @pl.when(jnp.logical_not(jnp.min(least[...]) > TINY))
    def _():
        clear(best, mixed)
        each_slot(
            counts,
            lambda slot: fine_slot(
                slot, counts, blocks, gains, work, values, best, weights, mixed, lam_out
            ),
        )


def fine_slot(slot, counts, blocks, gains, work, values, best, weights=None, mixed=None, lam_out=None):
    potential = slot_potential(slot, counts, blocks, values)
    mask = eye(128)
    highest = jnp.full((8, WIDTH), lowest, jnp.float32)
    lams = []
    for k in range(CHUNKS):
        at = slice(k * CHUNK, (k + 1) * CHUNK)
        scores = gains[slot, at, :] + potential
        lam = row_lse_chunk(scores)
        scores = scores - lam
        work[at, :] = scores
        highest = jnp.maximum(highest, jnp.max(scores.reshape(CHUNK // 8, 8, WIDTH), axis=0))
        lams.append(lam)
    highest = jnp.max(highest, axis=0, keepdims=True)
    total = jnp.zeros((8, WIDTH), jnp.float32)
    if weights is not None:
        w_row = weights[slot]
        w_cols = [to_column(w_row[:, h * 128 : (h + 1) * 128], mask) for h in range(2)]
        w_col = jnp.concatenate(w_cols, axis=0)
        weighted = jnp.zeros((8, WIDTH), jnp.float32)
    for k in range(CHUNKS):
        at = slice(k * CHUNK, (k + 1) * CHUNK)
        value = jnp.exp2(work[at, :] - highest)
        total = total + jnp.sum(value.reshape(CHUNK // 8, 8, WIDTH), axis=0)
        if weights is not None:
            value = value * w_col[at]
            weighted = weighted + jnp.sum(value.reshape(CHUNK // 8, 8, WIDTH), axis=0)
    total = jnp.sum(total, axis=0, keepdims=True)
    result = highest + jnp.log2(total)
    mean = None if weights is None else jnp.sum(weighted, axis=0, keepdims=True) / total
    merge_columns(slot, counts, blocks, values, best, mixed, result, mean)
    if lam_out is not None:
        for h in range(2):
            at = slice(h * 128, (h + 1) * 128)
            lam_out[slot, :, at] = to_row(jnp.concatenate(lams[h * CHUNKS // 2 : (h + 1) * CHUNKS // 2], axis=0), mask)


def clear(best, mixed=None):
    best[...] = jnp.full(best.shape, lowest, jnp.float32)
    if mixed is not None:
        mixed[...] = jnp.zeros(mixed.shape, jnp.float32)


def each_slot(counts, body, copies=None):
    def step(slot, carry):
        @pl.when(counts[slot] > 0)
        def _():
            if copies is not None:
                for copy in copies(slot):
                    copy.wait()
            body(slot)

        return carry

    lax.fori_loop(0, N_COLS, step, 0)


def first_pass_kernel(
    base, counts, blocks, p0, p1, p2, p3, labels, gains, best, kept, values, work, least, sums, cols
):
    cluster_values = -lse_list([p0[...], p1[...], p2[...], p3[...]])
    index = labels[...] - base[0]
    found = jnp.zeros((128, 128), jnp.float32)
    for part in range(4):
        row = cluster_values[:, part * 128 : (part + 1) * 128]
        picked = jnp.take_along_axis(
            jnp.broadcast_to(row, (128, 128)), index & 127, axis=1, mode="promise_in_bounds"
        )
        found = jnp.where(index >> 7 == part, picked, found)
    for chunk in range(128):
        at = slice(chunk % 2 * 128, (chunk % 2 + 1) * 128)
        values[chunk // 2, :, at] = found[chunk : chunk + 1, :]
    fine_pass(counts, blocks, gains, work, values, best, least, sums, cols)


def second_pass_kernel(
    counts, blocks, l0, l1, l2, l3, weights, gains, best, mixed, lam, kept, values, work, least, sums, cols
):
    values[...] = -lse_list([l0[...], l1[...], l2[...], l3[...]])
    fine_pass(counts, blocks, gains, work, values, best, least, sums, cols, weights, mixed, lam)


def adjoint_kernel(
    counts, blocks, l0, l1, l2, l3, lam, halves, weights, col_weights, gains,
    potential_out, back, values,
):
    total = lse_list([l0[...], l1[...], l2[...], l3[...]])
    values[...] = -total
    potential_out[...] = total * (-1.0 / SCALE)
    back[...] = jnp.zeros(back.shape, jnp.float32)
    mask = eye(128)

    def body(slot):
        potential = slot_potential(slot, counts, blocks, values)
        spread = jnp.concatenate(
            [col_weights[blocks[slot * ACT + a]] for a in range(ACT)], axis=1
        )
        for h in range(2):
            half = slice(h * 128, (h + 1) * 128)
            shift = to_column(lam[slot, :, half], mask)
            sums, crossed = [], []
            for k in range(128 // CHUNK):
                at = slice(h * 128 + k * CHUNK, h * 128 + (k + 1) * CHUNK)
                scores = gains[slot, at, :] + potential
                entries = jnp.exp2(scores - shift[k * CHUNK : (k + 1) * CHUNK])
                sums.append(jnp.sum(entries, axis=1, keepdims=True))
                crossed.append(jnp.sum(entries * spread, axis=1, keepdims=True))
            mass = to_row(jnp.concatenate(sums, axis=0), mask)
            cross = to_row(jnp.concatenate(crossed, axis=0), mask)
            back[slot, :, half] = halves[slot, :, half] - lam[slot, :, half] * (1.0 / SCALE)
            back[slot, :, BLOCK + h * 128 : BLOCK + (h + 1) * 128] = (
                weights[slot, :, half] * mass + cross
            )

    each_slot(counts, body)


def plan_kernel(row, col, lists_hbm, counts_hbm, counts, blocks, owners, lists, found, sems):
    first = pl.multiple_of(row[0] * 128, 128)
    copies = [
        pltpu.make_async_copy(lists_hbm.at[:, pl.ds(first, 128)], lists, sems.at[0]),
        pltpu.make_async_copy(counts_hbm.at[row[0]], found, sems.at[1]),
    ]
    for copy in copies:
        copy.start()
    for copy in copies:
        copy.wait()
    for q in range(RBD):
        owners[q] = lists[0, col[0] * RBD + q] >> 6

    def fill(slot, carry):
        count = jnp.int32(0)
        chosen = [jnp.int32(0)] * ACT
        for q in range(RBD):
            index = slot * RBD + q
            here = (lists[0, index] >> 6) == col[0]
            count = jnp.where(here, found[index], count)
            chosen = [
                jnp.where(here, lists[a, index] & (CBD - 1), old) for a, old in enumerate(chosen)
            ]
        counts[slot] = count
        for a in range(ACT):
            blocks[slot * ACT + a] = chosen[a]
        return carry

    lax.fori_loop(0, N_COLS, fill, 0)


def home_kernel(owners, back, potential, adjoint):
    for q in range(RBD):
        got = back[owners[q]]
        for h in range(2):
            at = slice(2 * q + h, 2 * q + h + 1)
            potential[at, :] = got[:, h * 128 : (h + 1) * 128]
            adjoint[at, :] = got[:, BLOCK + h * 128 : BLOCK + (h + 1) * 128]


def spread_kernel(owners, points, weights, out):
    for q in range(RBD):
        owner = owners[q]
        out[owner, :BLOCK, :] = points[q * BLOCK : (q + 1) * BLOCK, :]
        rest = weights[q]
        pieces = []
        for _ in range(3):
            piece = rest.astype(jnp.bfloat16)
            rest = rest - piece.astype(jnp.float32)
            pieces.append(piece.astype(jnp.float32))
        pieces.append(jnp.zeros((10, D), jnp.float32))
        out[owner, BLOCK:, :] = jnp.concatenate(pieces, axis=0).astype(jnp.bfloat16)


def cost(flops):
    return pl.CostEstimate(flops=int(flops), transcendentals=0, bytes_accessed=4 << 20)


def call(kernel, out_shape, in_specs, scratch=(), flops=1e8, **kw):
    out_specs = jax.tree.map(lambda _: VM, out_shape, is_leaf=lambda x: hasattr(x, "shape"))
    return pl.pallas_call(
        kernel,
        out_shape=out_shape,
        in_specs=in_specs,
        out_specs=out_specs,
        scratch_shapes=list(scratch),
        compiler_params=pltpu.CompilerParams(vmem_limit_bytes=24 << 20),
        cost_estimate=cost(flops),
        **kw,
    )


def exchange(x, axis):
    return lax.all_to_all(x, axis, split_axis=0, concat_axis=0, tiled=True)


def partner(x, axis, step):
    n = lax.axis_size(axis)
    return lax.ppermute(x, axis, [(k, k ^ step) for k in range(n)])


def four_along(x, axis):
    found = [x]
    for step in (1, 2, 3):
        found.append(partner(x, axis, step))
    return found


def four_along_x(x):
    return [in_vmem(part) for part in four_along(x, "x")]


def on_device(
    source_points,
    target_points,
    source_cluster,
    target_cluster,
    active_blocks,
    active_count,
    row_weight,
    col_weight,
):
    row_index = lax.axis_index(ROWS)
    col_index = lax.axis_index(COLS)
    device = row_index * N_COLS + col_index

    source_base = (CL_DEV * device).reshape(1).astype(jnp.int32)
    target_base = (N_TGT * col_index).reshape(1).astype(jnp.int32)
    packed = call(
        source_means_kernel, vmem_shape(N_COLS, CL_DEV + 8, D), [SM, VM, VM]
    )(source_base, in_hbm(source_points), in_hbm(source_cluster.reshape(1, PTS_SRC)))
    gathered = exchange(packed, COLS)

    row_weights = row_weight.reshape(RBD, 2, 128)
    col_weights = col_weight.reshape(CBD, 1, BLOCK)
    counts, blocks, owners = pl.pallas_call(
        plan_kernel,
        out_shape=tuple(jax.ShapeDtypeStruct((n,), jnp.int32) for n in (N_COLS, N_COLS * ACT, RBD)),
        in_specs=[SM, SM, ANY, ANY],
        out_specs=(SM, SM, SM),
        scratch_shapes=[
            pltpu.SMEM((ACT, 128), jnp.int32),
            pltpu.SMEM((128,), jnp.int32),
            pltpu.SemaphoreType.DMA((2,)),
        ],
        name="plan",
    )(
        row_index.reshape(1).astype(jnp.int32),
        col_index.reshape(1).astype(jnp.int32),
        in_hbm(active_blocks.T),
        in_hbm(active_count.reshape(8, 128)),
    )
    sent_points = call(
        spread_kernel, vmem_shape(N_COLS, PACKED, D, dtype=jnp.bfloat16), [SM, VM, VM]
    )(owners, in_hbm(source_points), in_hbm(row_weights))
    points_here = exchange(sent_points, COLS)

    firsts = target_cluster.reshape(128, 128)[:, 0] - target_base
    target_means, target_logs, norms = call(
        target_stats_kernel,
        (vmem_shape(N_TGT, D), vmem_shape(1, N_TGT), vmem_shape(CBD, 1, BLOCK)),
        [SM, SM, VM, ANY],
        [
            pltpu.VMEM((N_TGT + PIECE, 2 * D), jnp.float32),
            pltpu.VMEM((PTS_TGT, D), jnp.bfloat16),
            pltpu.SemaphoreType.DMA((8,)),
        ],
        flops=1e9,
    )(target_base, firsts, target_cluster.reshape(CBD, 1, BLOCK), in_hbm(target_points))

    gains, source_logs, partial = call(
        coarse_start_kernel,
        (vmem_shape(N_SRC, N_TGT), vmem_shape(8, 128), vmem_shape(N_COLS, 8, 128)),
        [VM, VM],
        flops=1e9,
    )(in_vmem(gathered), in_vmem(target_means))
    gains, source_logs, target_logs = in_vmem(gains), in_vmem(source_logs), in_vmem(target_logs)

    def coarse_cols(parts, out_shape):
        return call(
            coarse_cols_kernel,
            out_shape,
            [VM] * (len(parts) + 2),
            [pltpu.VMEM((N_SRC, N_TGT), jnp.float32)],
        )(*[in_vmem(part) for part in parts], source_logs, gains)

    def coarse_rows(parts):
        return call(
            coarse_rows_kernel, vmem_shape(N_COLS, 8, 128), [VM] * (len(parts) + 2)
        )(*[in_vmem(part) for part in parts], target_logs, gains)

    for sweep in range(ITER_C):
        source_parts = [exchange(partial, COLS)]
        permuted = sweep in (0, ITER_C - 1)
        cols_shape = vmem_shape(1, N_TGT) if permuted else vmem_shape(N_ROWS, 1, N_TGT)
        cols_partial = coarse_cols(source_parts, cols_shape)
        if permuted:
            pair = lse_list([cols_partial, partner(cols_partial, "core", 1)])
            target_parts = four_along(pair, "x")
        else:
            target_parts = [exchange(cols_partial, ROWS)]
        if sweep + 1 < ITER_C:
            partial = coarse_rows(target_parts)

    slot_row = vmem_shape(N_COLS, 1, BLOCK)
    fine_gains, halves, weights = call(
        products_kernel,
        (vmem_shape(N_COLS, BLOCK, WIDTH), slot_row, slot_row),
        [SM, SM, VM, ANY, ANY],
        [
            pltpu.VMEM((N_COLS, PACKED, D), jnp.bfloat16),
            pltpu.VMEM((N_COLS * ACT, BLOCK, D), jnp.bfloat16),
            pltpu.SemaphoreType.DMA((N_COLS, ACT + 1)),
        ],
        flops=1e9,
    )(counts, blocks, in_vmem(norms), in_hbm(points_here), in_hbm(target_points))
    fine_gains, halves, weights = in_vmem(fine_gains), in_vmem(halves), in_vmem(weights)
    column = vmem_shape(CBD, 1, BLOCK)
    values_scratch = pltpu.VMEM((CBD, 1, BLOCK), jnp.float32)
    work_scratch = pltpu.VMEM((BLOCK, WIDTH), jnp.float32)
    fast_scratch = [
        pltpu.VMEM((1, BLOCK), jnp.float32),
        pltpu.VMEM((16, WIDTH), jnp.float32),
        pltpu.VMEM((BLOCK, 8), jnp.float32),
    ]
    fine_shape = vmem_shape(N_COLS, BLOCK, WIDTH)
    best, fine_gains = call(
        first_pass_kernel,
        (column, fine_shape),
        [SM, SM, SM, VM, VM, VM, VM, VM, VM],
        [values_scratch, work_scratch, *fast_scratch],
        input_output_aliases={8: 1},
    )(
        target_base,
        counts,
        blocks,
        *[in_vmem(part) for part in target_parts],
        target_cluster.reshape(128, 128),
        fine_gains,
    )
    best = lse_list([best, partner(best, "core", 1)])

    best, mixed, lam, fine_gains = call(
        second_pass_kernel,
        (column, column, slot_row, fine_shape),
        [SM, SM, VM, VM, VM, VM, VM, VM],
        [values_scratch, work_scratch, *fast_scratch],
        input_output_aliases={7: 3},
    )(counts, blocks, *four_along_x(best), weights, in_vmem(fine_gains))
    other = partner(best, "core", 1)
    other_mixed = partner(mixed, "core", 1)
    total = lse_list([best, other])
    mixed = mixed * jnp.exp2(best - total) + other_mixed * jnp.exp2(other - total)
    best_parts = four_along(total, "x")
    mixed_parts = four_along(mixed, "x")

    col_potential, back = call(
        adjoint_kernel,
        (shape(CBD, 1, BLOCK), vmem_shape(N_COLS, 1, 2 * BLOCK)),
        [SM, SM, VM, VM, VM, VM, VM, VM, VM, VM, VM],
        [values_scratch],
    )(
        counts, blocks, *[in_vmem(part) for part in best_parts], in_vmem(lam), halves,
        weights, col_weights, in_vmem(fine_gains),
    )
    total = lse_list(best_parts)
    mixed = [m * jnp.exp2(part - total) for m, part in zip(mixed_parts, best_parts)]
    col_adjoint = ((mixed[0] + mixed[1]) + (mixed[2] + mixed[3])) + col_weights
    back = exchange(back, COLS)
    row_potential, row_adjoint = call(
        home_kernel, (shape(16, 128), shape(16, 128)), [SM, VM]
    )(owners, in_vmem(back))
    return (
        row_potential.reshape(-1),
        col_potential.reshape(-1),
        row_adjoint.reshape(-1),
        col_adjoint.reshape(-1),
    )


def solution(mesh):
    split = Mesh(mesh.devices.reshape(4, 2, 4, 4), ALL)
    placed = (
        P(ALL, None),
        P(COLS, None),
        P(ALL),
        P(COLS),
        P(),
        P(),
        P(ALL),
        P(COLS),
    )
    return jax.shard_map(
        on_device,
        mesh=split,
        in_specs=placed,
        out_specs=(P(ALL), P(COLS), P(ALL), P(COLS)),
        check_vma=False,
    )
```

```python
import jax
import jax.numpy as jnp
from jax import lax
from jax.experimental import pallas as pl
from jax.experimental.pallas import tpu as pltpu
from jax.sharding import Mesh
from jax.sharding import PartitionSpec as P


D = 128
BLOCK = 256
ACT = 4
ITER_C = 4
CL_DEV = 64
RBD = 8
CBD = 64
ROWS = ("x", "core")
COLS = ("y", "z")
ALL = ("x", "core", "y", "z")
N_ROWS = 8
N_COLS = 16
N_SRC = CL_DEV * N_COLS
N_TGT = 512
PTS_SRC = 2048
PTS_TGT = 16384
PIECE = 32
TINY = 2.0**-80
PACKED = BLOCK + 16

SCALE = 2.8853900817779268
lowest = -1.0e30
HI = lax.Precision.HIGHEST
NT = (((1,), (1,)), ((), ()))

VM = pl.BlockSpec(memory_space=pltpu.VMEM)
SM = pl.BlockSpec(memory_space=pltpu.SMEM)
ANY = pl.BlockSpec(memory_space=pl.ANY)


def vmem_shape(*dims, dtype=jnp.float32):
    return pltpu.VMEM(dims, dtype)


def in_vmem(x):
    return pltpu.with_memory_space_constraint(x, pltpu.VMEM)


def shape(*dims):
    return pltpu.HBM(dims, jnp.float32)


def in_hbm(x):
    return pltpu.with_memory_space_constraint(x, pltpu.HBM)


def eye(rows, shift=0):
    return lax.broadcasted_iota(jnp.int32, (rows, 128), 0) + shift == lax.broadcasted_iota(
        jnp.int32, (rows, 128), 1
    )


def to_row(column, mask):
    return jnp.sum(jnp.where(mask, column, 0.0), axis=0, keepdims=True)


def to_column(row, mask):
    return jnp.sum(jnp.where(mask, row, 0.0), axis=1, keepdims=True)


def lse_list(parts):
    highest = parts[0]
    for part in parts[1:]:
        highest = jnp.maximum(highest, part)
    terms = [jnp.exp2(part - highest) for part in parts]
    while len(terms) > 1:
        terms = [terms[k] + terms[k + 1] for k in range(0, len(terms), 2)]
    return highest + jnp.log2(terms[0])


def one_hot(labels, rows):
    hit = lax.broadcasted_iota(jnp.int32, (rows, labels.shape[1]), 0) == labels
    return jnp.where(hit, 1.0, 0.0).astype(jnp.bfloat16)


def totals_and_counts(hits, points):
    both = jnp.concatenate([points, jnp.ones(points.shape, jnp.bfloat16)], axis=1)
    return jnp.dot(hits, both, preferred_element_type=jnp.float32)


def square_sums(points, factor):
    wide = points.astype(jnp.float32)
    square = wide * wide
    high = square.astype(jnp.bfloat16)
    low = (square - high.astype(jnp.float32)).astype(jnp.bfloat16)
    ones = jnp.full((8, 2 * D), 1.0, jnp.bfloat16)
    both = jnp.concatenate([high, low], axis=1)
    return factor * lax.dot_general(ones, both, NT, preferred_element_type=jnp.float32)[:1]


def source_means_kernel(base, points, labels, out):
    both = totals_and_counts(one_hot(labels[...] - base[0], CL_DEV), points[...])
    counts = both[:, D:]
    means = both[:, :D] / counts
    low = to_row(counts, eye(CL_DEV))
    high = to_row(counts, eye(CL_DEV, 64))
    tail = lax.broadcasted_iota(jnp.int32, (8, 128), 0)
    tail = jnp.where(tail == 0, low, jnp.where(tail == 1, high, 0.0))
    for peer in range(N_COLS):
        out[peer, :CL_DEV, :] = means
        out[peer, CL_DEV:, :] = tail


def target_stats_kernel(base, firsts, labels, y_hbm, means, logs, norms, acc, ys, sems):
    copies = [
        pltpu.make_async_copy(
            y_hbm.at[k * 2048 : (k + 1) * 2048, :], ys.at[k * 2048 : (k + 1) * 2048, :], sems.at[k]
        )
        for k in range(8)
    ]
    for copy in copies:
        copy.start()
    acc[...] = jnp.zeros_like(acc)

    def piece(chunk, start, points_here):
        hits = one_hot(labels[chunk] - (start + base[0]), PIECE)
        window = pl.ds(pl.multiple_of(start, 8), PIECE)
        acc[window, :] += totals_and_counts(hits, points_here)

    for step in range(8):
        copies[step].wait()

        def some(n, most, step=step):
            for k in range(4):
                chunk = step * 8 + n * 4 + k
                points = ys[pl.ds(pl.multiple_of(chunk * BLOCK, BLOCK), BLOCK), :]
                start = firsts[2 * chunk] // 8 * 8
                piece(chunk, start, points)
                beyond = firsts[jnp.minimum(2 * chunk + 2, 127)]
                beyond = jnp.where(chunk < CBD - 1, beyond, N_TGT - 1)
                most = jnp.maximum(most, (beyond - start) // PIECE)
                norms[chunk] = square_sums(points, 0.5 * SCALE)
            return most

        most = lax.fori_loop(0, 2, some, 0)

        @pl.when(most > 0)
        def _(step=step):
            def chunk_rest(chunk, carry):
                start = firsts[2 * chunk] // 8 * 8
                beyond = firsts[jnp.minimum(2 * chunk + 2, 127)]
                beyond = jnp.where(chunk < CBD - 1, beyond, N_TGT - 1)

                def more(k, carry):
                    points = ys[pl.ds(pl.multiple_of(chunk * BLOCK, BLOCK), BLOCK), :]
                    piece(chunk, start + k * PIECE, points)
                    return carry

                lax.fori_loop(1, (beyond - start) // PIECE + 1, more, 0)
                return carry

            lax.fori_loop(step * 8, step * 8 + 8, chunk_rest, 0)

    mask = eye(128)
    for part in range(4):
        at = slice(part * 128, (part + 1) * 128)
        counts = acc[at, D:]
        means[at, :] = acc[at, :D] / counts
        logs[:, at] = jnp.log2(to_row(counts, mask))


def row_lse_chunk(scores):
    highest = jnp.max(scores, axis=1, keepdims=True)
    return highest + jnp.log2(jnp.sum(jnp.exp2(scores - highest), axis=1, keepdims=True))


def coarse_start_kernel(gathered, targets, gains, source_logs, out):
    mask = eye(128)
    y = targets[...]
    half_y = 0.5 * jnp.sum(y * y, axis=1, keepdims=True)
    half_y = jnp.concatenate(
        [to_row(half_y[k * 128 : (k + 1) * 128], mask) for k in range(4)], axis=1
    )
    for part in range(8):
        x = jnp.concatenate(
            [gathered[2 * part, :CL_DEV, :], gathered[2 * part + 1, :CL_DEV, :]], axis=0
        )
        counts = gathered[2 * part, 64:65, :] + gathered[2 * part + 1, 65:66, :]
        source_logs[part : part + 1, :] = jnp.log2(counts)
        half_x = 0.5 * jnp.sum(x * x, axis=1, keepdims=True)
        products = lax.dot_general(x, y, NT, precision=HI, preferred_element_type=jnp.float32)
        gain = SCALE * (products - (half_x + half_y))
        gains[part * 128 : (part + 1) * 128, :] = gain
        out[0, part : part + 1, :] = to_row(row_lse_chunk(gain), mask)
    first = out[0]
    for peer in range(1, N_COLS):
        out[peer] = first


def parts_of(refs):
    if len(refs) == 1:
        return [refs[0][k] for k in range(refs[0].shape[0])]
    return [ref[...] for ref in refs]


def coarse_rows_kernel(*refs):
    *gathered, target_logs, gains, out = refs
    mask = eye(128)
    potential = target_logs[...] - lse_list(parts_of(gathered))
    for part in range(8):
        pieces = []
        for piece in range(1):
            at = part * 128 + piece * 128
            pieces.append(row_lse_chunk(gains[at : at + 128, :] + potential))
        out[0, part : part + 1, :] = to_row(jnp.concatenate(pieces, axis=0), mask)
    first = out[0]
    for peer in range(1, N_COLS):
        out[peer] = first


def coarse_cols_kernel(*refs):
    *gathered, source_logs, gains, out, scores = refs
    mask = eye(128)
    potential = source_logs[...] - lse_list(parts_of(gathered))
    highest = jnp.full((8, N_TGT), lowest, jnp.float32)
    for part in range(8):
        at = slice(part * 128, (part + 1) * 128)
        value = gains[at, :] + to_column(potential[part : part + 1, :], mask)
        scores[at, :] = value
        highest = jnp.maximum(highest, jnp.max(value.reshape(16, 8, N_TGT), axis=0))
    highest = jnp.max(highest, axis=0, keepdims=True)
    total = jnp.zeros((8, N_TGT), jnp.float32)
    for part in range(8):
        at = slice(part * 128, (part + 1) * 128)
        value = jnp.exp2(scores[at, :] - highest)
        total = total + jnp.sum(value.reshape(16, 8, N_TGT), axis=0)
    result = highest + jnp.log2(jnp.sum(total, axis=0, keepdims=True))
    if len(out.shape) == 2:
        out[...] = result
    else:
        for peer in range(N_ROWS):
            out[peer] = result


def start_copies(counts, blocks, x_hbm, y_hbm, xs, ys, sems):
    def copies(slot):
        found = [pltpu.make_async_copy(x_hbm.at[slot], xs.at[slot], sems.at[slot, ACT])]
        for a in range(ACT):
            first = pl.multiple_of(blocks[slot * ACT + a] * BLOCK, BLOCK)
            found.append(
                pltpu.make_async_copy(
                    y_hbm.at[pl.ds(first, BLOCK), :], ys.at[slot * ACT + a], sems.at[slot, a]
                )
            )
        return found

    def begin(slot, carry):
        @pl.when(counts[slot] > 0)
        def _():
            for copy in copies(slot):
                copy.start()

        return carry

    lax.fori_loop(0, N_COLS, begin, 0)
    return copies


def products_kernel(counts, blocks, order, norms, x_hbm, y_hbm, gains, halves, weights, xs, ys, sems):
    copies = start_copies(counts, blocks, x_hbm, y_hbm, xs, ys, sems)

    def body(slot):
        x = xs[slot, :BLOCK, :]
        tail = xs[slot, BLOCK:, :].astype(jnp.float32)
        halves[slot] = square_sums(x, 0.5)
        for h in range(2):
            at = slice(h * 128, (h + 1) * 128)
            weights[slot, :, at] = (tail[h : h + 1] + tail[h + 2 : h + 3]) + tail[h + 4 : h + 5]
        for a in range(ACT):
            products = lax.dot_general(
                x, ys[slot * ACT + a], NT, preferred_element_type=jnp.float32
            )
            gains[slot, :, a * BLOCK : (a + 1) * BLOCK] = (
                SCALE * products - norms[blocks[slot * ACT + a]]
            )

    slot_pairs(order, body, copies)


def slot_potential(slot, counts, blocks, values):
    rows = []
    for a in range(ACT):
        row = values[blocks[slot * ACT + a]]
        rows.append(jnp.where(a < counts[slot], row, lowest))
    return jnp.concatenate(rows, axis=1)


CHUNK = 8
CHUNKS = BLOCK // CHUNK
WIDTH = ACT * BLOCK


def merge_columns(slot, counts, blocks, values, best, mixed, result, mean):
    for a in range(ACT):
        block = blocks[slot * ACT + a]
        at = slice(a * BLOCK, (a + 1) * BLOCK)
        here = jnp.where(a < counts[slot], result[:, at] - values[block], lowest)
        old = best[block]
        top = jnp.maximum(old, here)
        old_part, new_part = jnp.exp2(old - top), jnp.exp2(here - top)
        both = old_part + new_part
        best[block] = top + jnp.log2(both)
        if mean is not None:
            part = jnp.where(a < counts[slot], mean[:, at], 0.0)
            mixed[block] = (mixed[block] * old_part + part * new_part) / both


GROUP = 256
FAST = 8


def fast_slot(slot, counts, blocks, gains, values, best, least, sums, cols, weights=None, mixed=None, lam_out=None):
    potential = slot_potential(slot, counts, blocks, values)
    mask = eye(128)
    if weights is not None:
        w_row = weights[slot]
        for h in range(2):
            at = slice(h * 128, (h + 1) * 128)
            cols[at, 0:1] = to_column(w_row[:, at], mask)
    sums[...] = jnp.zeros(sums.shape, jnp.float32)

    def group(step, carry):
        total = sums[:8, :]
        weighted = sums[8:, :]
        for k in range(GROUP // FAST):
            at = pl.ds(pl.multiple_of(step * GROUP + k * FAST, FAST), FAST)
            scores = gains[slot, at, :] + potential
            highest = jnp.max(scores, axis=1, keepdims=True)
            entries = jnp.exp2(scores - highest)
            mass = jnp.sum(entries, axis=1, keepdims=True)
            if lam_out is not None:
                cols[at, 1:2] = highest + jnp.log2(mass)
            scale = 1.0 / mass
            part = (entries * scale).reshape(FAST // 8, 8, WIDTH)
            total = total + jnp.sum(part, axis=0)
            if weights is not None:
                part = (entries * (scale * cols[at, 0:1])).reshape(FAST // 8, 8, WIDTH)
                weighted = weighted + jnp.sum(part, axis=0)
        sums[:8, :] = total
        if weights is not None:
            sums[8:, :] = weighted
        return carry

    lax.fori_loop(0, BLOCK // GROUP, group, 0)
    total = jnp.sum(sums[:8, :], axis=0, keepdims=True)
    mean = None if weights is None else jnp.sum(sums[8:, :], axis=0, keepdims=True) / total
    for a in range(ACT):
        part = jnp.where(a < counts[slot], total[:, a * BLOCK : (a + 1) * BLOCK], 1.0)
        least[...] = jnp.minimum(least[...], part)
    merge_columns(slot, counts, blocks, values, best, mixed, jnp.log2(total), mean)
    if lam_out is not None:
        for h in range(2):
            at = slice(h * 128, (h + 1) * 128)
            lam_out[slot, :, at] = to_row(cols[at, 1:2], mask)


def fine_pass(counts, blocks, gains, work, values, best, least, sums, cols, weights=None, mixed=None, lam_out=None):
    clear(best, mixed)
    least[...] = jnp.ones(least.shape, jnp.float32)
    each_slot(
        counts,
        lambda slot: fast_slot(
            slot, counts, blocks, gains, values, best, least, sums, cols, weights, mixed, lam_out
        ),
    )

    @pl.when(jnp.logical_not(jnp.min(least[...]) > TINY))
    def _():
        clear(best, mixed)
        each_slot(
            counts,
            lambda slot: fine_slot(
                slot, counts, blocks, gains, work, values, best, weights, mixed, lam_out
            ),
        )


def fine_slot(slot, counts, blocks, gains, work, values, best, weights=None, mixed=None, lam_out=None):
    potential = slot_potential(slot, counts, blocks, values)
    mask = eye(128)
    highest = jnp.full((8, WIDTH), lowest, jnp.float32)
    lams = []
    for k in range(CHUNKS):
        at = slice(k * CHUNK, (k + 1) * CHUNK)
        scores = gains[slot, at, :] + potential
        lam = row_lse_chunk(scores)
        scores = scores - lam
        work[at, :] = scores
        highest = jnp.maximum(highest, jnp.max(scores.reshape(CHUNK // 8, 8, WIDTH), axis=0))
        lams.append(lam)
    highest = jnp.max(highest, axis=0, keepdims=True)
    total = jnp.zeros((8, WIDTH), jnp.float32)
    if weights is not None:
        w_row = weights[slot]
        w_cols = [to_column(w_row[:, h * 128 : (h + 1) * 128], mask) for h in range(2)]
        w_col = jnp.concatenate(w_cols, axis=0)
        weighted = jnp.zeros((8, WIDTH), jnp.float32)
    for k in range(CHUNKS):
        at = slice(k * CHUNK, (k + 1) * CHUNK)
        value = jnp.exp2(work[at, :] - highest)
        total = total + jnp.sum(value.reshape(CHUNK // 8, 8, WIDTH), axis=0)
        if weights is not None:
            value = value * w_col[at]
            weighted = weighted + jnp.sum(value.reshape(CHUNK // 8, 8, WIDTH), axis=0)
    total = jnp.sum(total, axis=0, keepdims=True)
    result = highest + jnp.log2(total)
    mean = None if weights is None else jnp.sum(weighted, axis=0, keepdims=True) / total
    merge_columns(slot, counts, blocks, values, best, mixed, result, mean)
    if lam_out is not None:
        for h in range(2):
            at = slice(h * 128, (h + 1) * 128)
            lam_out[slot, :, at] = to_row(jnp.concatenate(lams[h * CHUNKS // 2 : (h + 1) * CHUNKS // 2], axis=0), mask)


def slot_pairs(order, body, copies=None):
    used = order[N_COLS + 1]

    def step(pair, carry):
        first, second = order[2 * pair], order[2 * pair + 1]
        if copies is not None:
            for copy in copies(first):
                copy.wait()

            @pl.when(2 * pair + 1 < used)
            def _():
                for copy in copies(second):
                    copy.wait()

        body(first)
        body(second)
        return carry

    lax.fori_loop(0, (used + 1) // 2, step, 0)


def clear(best, mixed=None):
    best[...] = jnp.full(best.shape, lowest, jnp.float32)
    if mixed is not None:
        mixed[...] = jnp.zeros(mixed.shape, jnp.float32)


def each_slot(counts, body, copies=None):
    def step(slot, carry):
        @pl.when(counts[slot] > 0)
        def _():
            if copies is not None:
                for copy in copies(slot):
                    copy.wait()
            body(slot)

        return carry

    lax.fori_loop(0, N_COLS, step, 0)


def first_pass_kernel(
    base, counts, blocks, p0, p1, p2, p3, labels, gains, best, kept, values, work, least, sums, cols
):
    cluster_values = -lse_list([p0[...], p1[...], p2[...], p3[...]])
    index = labels[...] - base[0]
    found = jnp.zeros((128, 128), jnp.float32)
    for part in range(4):
        row = cluster_values[:, part * 128 : (part + 1) * 128]
        picked = jnp.take_along_axis(
            jnp.broadcast_to(row, (128, 128)), index & 127, axis=1, mode="promise_in_bounds"
        )
        found = jnp.where(index >> 7 == part, picked, found)
    for chunk in range(128):
        at = slice(chunk % 2 * 128, (chunk % 2 + 1) * 128)
        values[chunk // 2, :, at] = found[chunk : chunk + 1, :]
    fine_pass(counts, blocks, gains, work, values, best, least, sums, cols)


def second_pass_kernel(
    counts, blocks, l0, l1, l2, l3, weights, gains, best, mixed, lam, kept, values, work, least, sums, cols
):
    values[...] = -lse_list([l0[...], l1[...], l2[...], l3[...]])
    fine_pass(counts, blocks, gains, work, values, best, least, sums, cols, weights, mixed, lam)


def adjoint_kernel(
    counts, blocks, order, l0, l1, l2, l3, lam, halves, weights, col_weights, gains,
    potential_out, back, values,
):
    total = lse_list([l0[...], l1[...], l2[...], l3[...]])
    values[...] = -total
    potential_out[...] = total * (-1.0 / SCALE)
    back[...] = jnp.zeros(back.shape, jnp.float32)
    mask = eye(128)

    def body(slot):
        potential = slot_potential(slot, counts, blocks, values)
        spread = jnp.concatenate(
            [col_weights[blocks[slot * ACT + a]] for a in range(ACT)], axis=1
        )
        for h in range(2):
            half = slice(h * 128, (h + 1) * 128)
            shift = to_column(lam[slot, :, half], mask)
            sums, crossed = [], []
            for k in range(128 // CHUNK):
                at = slice(h * 128 + k * CHUNK, h * 128 + (k + 1) * CHUNK)
                scores = gains[slot, at, :] + potential
                entries = jnp.exp2(scores - shift[k * CHUNK : (k + 1) * CHUNK])
                sums.append(jnp.sum(entries, axis=1, keepdims=True))
                crossed.append(jnp.sum(entries * spread, axis=1, keepdims=True))
            mass = to_row(jnp.concatenate(sums, axis=0), mask)
            cross = to_row(jnp.concatenate(crossed, axis=0), mask)
            back[slot, :, half] = halves[slot, :, half] - lam[slot, :, half] * (1.0 / SCALE)
            back[slot, :, BLOCK + h * 128 : BLOCK + (h + 1) * 128] = (
                weights[slot, :, half] * mass + cross
            )

    slot_pairs(order, body)


def plan_kernel(
    row, col, lists_hbm, counts_hbm, counts, blocks, owners, order, lists, found, sems
):
    first = pl.multiple_of(row[0] * 128, 128)
    copies = [
        pltpu.make_async_copy(lists_hbm.at[:, pl.ds(first, 128)], lists, sems.at[0]),
        pltpu.make_async_copy(counts_hbm.at[row[0]], found, sems.at[1]),
    ]
    for copy in copies:
        copy.start()
    for copy in copies:
        copy.wait()
    for q in range(RBD):
        owners[q] = lists[0, col[0] * RBD + q] >> 6

    def fill(slot, place):
        count = jnp.int32(0)
        chosen = [jnp.int32(0)] * ACT
        for q in range(RBD):
            index = slot * RBD + q
            here = (lists[0, index] >> 6) == col[0]
            count = jnp.where(here, found[index], count)
            chosen = [
                jnp.where(here, lists[a, index] & (CBD - 1), old) for a, old in enumerate(chosen)
            ]
        counts[slot] = count
        for a in range(ACT):
            blocks[slot * ACT + a] = chosen[a]
        order[place] = slot
        return place + jnp.where(count > 0, 1, 0)

    used = lax.fori_loop(0, N_COLS, fill, jnp.int32(0))
    order[used] = order[jnp.maximum(used - 1, 0)]
    order[N_COLS + 1] = used


def home_kernel(owners, back, potential, adjoint):
    for q in range(RBD):
        got = back[owners[q]]
        for h in range(2):
            at = slice(2 * q + h, 2 * q + h + 1)
            potential[at, :] = got[:, h * 128 : (h + 1) * 128]
            adjoint[at, :] = got[:, BLOCK + h * 128 : BLOCK + (h + 1) * 128]


def spread_kernel(owners, points, weights, out):
    for q in range(RBD):
        owner = owners[q]
        out[owner, :BLOCK, :] = points[q * BLOCK : (q + 1) * BLOCK, :]
        rest = weights[q]
        pieces = []
        for _ in range(3):
            piece = rest.astype(jnp.bfloat16)
            rest = rest - piece.astype(jnp.float32)
            pieces.append(piece.astype(jnp.float32))
        pieces.append(jnp.zeros((10, D), jnp.float32))
        out[owner, BLOCK:, :] = jnp.concatenate(pieces, axis=0).astype(jnp.bfloat16)


def cost(flops):
    return pl.CostEstimate(flops=int(flops), transcendentals=0, bytes_accessed=4 << 20)


def call(kernel, out_shape, in_specs, scratch=(), flops=1e8, **kw):
    out_specs = jax.tree.map(lambda _: VM, out_shape, is_leaf=lambda x: hasattr(x, "shape"))
    return pl.pallas_call(
        kernel,
        out_shape=out_shape,
        in_specs=in_specs,
        out_specs=out_specs,
        scratch_shapes=list(scratch),
        compiler_params=pltpu.CompilerParams(vmem_limit_bytes=24 << 20),
        cost_estimate=cost(flops),
        **kw,
    )


def exchange(x, axis):
    return lax.all_to_all(x, axis, split_axis=0, concat_axis=0, tiled=True)


def partner(x, axis, step):
    n = lax.axis_size(axis)
    return lax.ppermute(x, axis, [(k, k ^ step) for k in range(n)])


def four_along(x, axis):
    found = [x]
    for step in (1, 2, 3):
        found.append(partner(x, axis, step))
    return found


def four_along_x(x):
    return [in_vmem(part) for part in four_along(x, "x")]


def on_device(
    source_points,
    target_points,
    source_cluster,
    target_cluster,
    active_blocks,
    active_count,
    row_weight,
    col_weight,
):
    row_index = lax.axis_index(ROWS)
    col_index = lax.axis_index(COLS)
    device = row_index * N_COLS + col_index

    source_base = (CL_DEV * device).reshape(1).astype(jnp.int32)
    target_base = (N_TGT * col_index).reshape(1).astype(jnp.int32)
    packed = call(
        source_means_kernel, vmem_shape(N_COLS, CL_DEV + 8, D), [SM, VM, VM]
    )(source_base, in_hbm(source_points), in_hbm(source_cluster.reshape(1, PTS_SRC)))
    gathered = exchange(packed, COLS)

    row_weights = row_weight.reshape(RBD, 2, 128)
    col_weights = col_weight.reshape(CBD, 1, BLOCK)
    counts, blocks, owners, order = pl.pallas_call(
        plan_kernel,
        out_shape=tuple(
            jax.ShapeDtypeStruct((n,), jnp.int32) for n in (N_COLS, N_COLS * ACT, RBD, N_COLS + 2)
        ),
        in_specs=[SM, SM, ANY, ANY],
        out_specs=(SM, SM, SM, SM),
        scratch_shapes=[
            pltpu.SMEM((ACT, 128), jnp.int32),
            pltpu.SMEM((128,), jnp.int32),
            pltpu.SemaphoreType.DMA((2,)),
        ],
        name="plan",
    )(
        row_index.reshape(1).astype(jnp.int32),
        col_index.reshape(1).astype(jnp.int32),
        in_hbm(active_blocks.T),
        in_hbm(active_count.reshape(8, 128)),
    )
    sent_points = call(
        spread_kernel, vmem_shape(N_COLS, PACKED, D, dtype=jnp.bfloat16), [SM, VM, VM]
    )(owners, in_hbm(source_points), in_hbm(row_weights))
    points_here = exchange(sent_points, COLS)

    firsts = target_cluster.reshape(128, 128)[:, 0] - target_base
    target_means, target_logs, norms = call(
        target_stats_kernel,
        (vmem_shape(N_TGT, D), vmem_shape(1, N_TGT), vmem_shape(CBD, 1, BLOCK)),
        [SM, SM, VM, ANY],
        [
            pltpu.VMEM((N_TGT + PIECE, 2 * D), jnp.float32),
            pltpu.VMEM((PTS_TGT, D), jnp.bfloat16),
            pltpu.SemaphoreType.DMA((8,)),
        ],
        flops=1e9,
    )(target_base, firsts, target_cluster.reshape(CBD, 1, BLOCK), in_hbm(target_points))

    gains, source_logs, partial = call(
        coarse_start_kernel,
        (vmem_shape(N_SRC, N_TGT), vmem_shape(8, 128), vmem_shape(N_COLS, 8, 128)),
        [VM, VM],
        flops=1e9,
    )(in_vmem(gathered), in_vmem(target_means))
    gains, source_logs, target_logs = in_vmem(gains), in_vmem(source_logs), in_vmem(target_logs)

    def coarse_cols(parts, out_shape):
        return call(
            coarse_cols_kernel,
            out_shape,
            [VM] * (len(parts) + 2),
            [pltpu.VMEM((N_SRC, N_TGT), jnp.float32)],
        )(*[in_vmem(part) for part in parts], source_logs, gains)

    def coarse_rows(parts):
        return call(
            coarse_rows_kernel, vmem_shape(N_COLS, 8, 128), [VM] * (len(parts) + 2)
        )(*[in_vmem(part) for part in parts], target_logs, gains)

    for sweep in range(ITER_C):
        source_parts = [exchange(partial, COLS)]
        permuted = sweep in (0, ITER_C - 1)
        cols_shape = vmem_shape(1, N_TGT) if permuted else vmem_shape(N_ROWS, 1, N_TGT)
        cols_partial = coarse_cols(source_parts, cols_shape)
        if permuted:
            pair = lse_list([cols_partial, partner(cols_partial, "core", 1)])
            target_parts = four_along(pair, "x")
        else:
            target_parts = [exchange(cols_partial, ROWS)]
        if sweep + 1 < ITER_C:
            partial = coarse_rows(target_parts)

    slot_row = vmem_shape(N_COLS, 1, BLOCK)
    fine_gains, halves, weights = call(
        products_kernel,
        (vmem_shape(N_COLS, BLOCK, WIDTH), slot_row, slot_row),
        [SM, SM, SM, VM, ANY, ANY],
        [
            pltpu.VMEM((N_COLS, PACKED, D), jnp.bfloat16),
            pltpu.VMEM((N_COLS * ACT, BLOCK, D), jnp.bfloat16),
            pltpu.SemaphoreType.DMA((N_COLS, ACT + 1)),
        ],
        flops=1e9,
    )(counts, blocks, order, in_vmem(norms), in_hbm(points_here), in_hbm(target_points))
    fine_gains, halves, weights = in_vmem(fine_gains), in_vmem(halves), in_vmem(weights)
    column = vmem_shape(CBD, 1, BLOCK)
    values_scratch = pltpu.VMEM((CBD, 1, BLOCK), jnp.float32)
    work_scratch = pltpu.VMEM((BLOCK, WIDTH), jnp.float32)
    fast_scratch = [
        pltpu.VMEM((1, BLOCK), jnp.float32),
        pltpu.VMEM((16, WIDTH), jnp.float32),
        pltpu.VMEM((BLOCK, 8), jnp.float32),
    ]
    fine_shape = vmem_shape(N_COLS, BLOCK, WIDTH)
    best, fine_gains = call(
        first_pass_kernel,
        (column, fine_shape),
        [SM, SM, SM, VM, VM, VM, VM, VM, VM],
        [values_scratch, work_scratch, *fast_scratch],
        input_output_aliases={8: 1},
    )(
        target_base,
        counts,
        blocks,
        *[in_vmem(part) for part in target_parts],
        target_cluster.reshape(128, 128),
        fine_gains,
    )
    best = lse_list([best, partner(best, "core", 1)])

    best, mixed, lam, fine_gains = call(
        second_pass_kernel,
        (column, column, slot_row, fine_shape),
        [SM, SM, VM, VM, VM, VM, VM, VM],
        [values_scratch, work_scratch, *fast_scratch],
        input_output_aliases={7: 3},
    )(counts, blocks, *four_along_x(best), weights, in_vmem(fine_gains))
    other = partner(best, "core", 1)
    other_mixed = partner(mixed, "core", 1)
    total = lse_list([best, other])
    mixed = mixed * jnp.exp2(best - total) + other_mixed * jnp.exp2(other - total)
    best_parts = four_along(total, "x")
    mixed_parts = four_along(mixed, "x")

    col_potential, back = call(
        adjoint_kernel,
        (shape(CBD, 1, BLOCK), vmem_shape(N_COLS, 1, 2 * BLOCK)),
        [SM, SM, SM, VM, VM, VM, VM, VM, VM, VM, VM, VM],
        [values_scratch],
    )(
        counts, blocks, order, *[in_vmem(part) for part in best_parts], in_vmem(lam), halves,
        weights, col_weights, in_vmem(fine_gains),
    )
    total = lse_list(best_parts)
    mixed = [m * jnp.exp2(part - total) for m, part in zip(mixed_parts, best_parts)]
    col_adjoint = ((mixed[0] + mixed[1]) + (mixed[2] + mixed[3])) + col_weights
    back = exchange(back, COLS)
    row_potential, row_adjoint = call(
        home_kernel, (shape(16, 128), shape(16, 128)), [SM, VM]
    )(owners, in_vmem(back))
    return (
        row_potential.reshape(-1),
        col_potential.reshape(-1),
        row_adjoint.reshape(-1),
        col_adjoint.reshape(-1),
    )


def solution(mesh):
    split = Mesh(mesh.devices.reshape(4, 2, 4, 4), ALL)
    placed = (
        P(ALL, None),
        P(COLS, None),
        P(ALL),
        P(COLS),
        P(),
        P(),
        P(ALL),
        P(COLS),
    )
    return jax.shard_map(
        on_device,
        mesh=split,
        in_specs=placed,
        out_specs=(P(ALL), P(COLS), P(ALL), P(COLS)),
        check_vma=False,
    )
```
